256 devices in a mesh: col: 8 (over z), row: 4 (over y), depth: 8 (over x, core).
Axes of the slice: x: 4, y: 4, z: 8, core: 2. Of those that a mesh axis runs over, the one named last changes fastest.
Arguments:
- a_mat: bfloat16 [12288, 24576], P(('depth', 'row', 'col'))
- b_mat: bfloat16 [24576, 12288], P(('depth', 'row', 'col'))
Outputs:
- output: bfloat16 [12288, 12288], P(('depth', 'row', 'col'))
All inputs are finite; a program needn't handle non-finite values.
Results may differ from the reference program's by a relative error of at most 0.001.
Values are sent between devices in bfloat16 or wider.
A program may use at most 768 MiB of HBM per device.

```python
import jax
import jax.numpy as jnp

D = 12288
F = 12288
TOKENS = 24576


def setup_inputs(seed: int = 0) -> dict:
    key_a, key_b = jax.random.split(jax.random.key(seed))
    a_vals = jax.random.normal(key_a, (D, TOKENS), jnp.float32)
    b_vals = jax.random.normal(key_b, (TOKENS, F), jnp.float32) * (TOKENS ** -0.5)
    return {"a_mat": a_vals.astype(jnp.bfloat16), "b_mat": b_vals.astype(jnp.bfloat16)}


def reference(a_mat, b_mat):
    product = jnp.dot(a_mat, b_mat, preferred_element_type=jnp.float32)
    return product.astype(jnp.bfloat16)
```

```python
import jax
import jax.numpy as jnp
from jax import lax
from jax.experimental import pallas as pl
from jax.experimental.pallas import tpu as pltpu
from jax.sharding import PartitionSpec as P

X = 4
Y = 4
Z = 8
NC = 6
STEPS = 7
FIRST = 24
TILES = NC * Y


def kernel(a_in, b_in, out, a_buf, b_buf, c_buf, rp, rm, fp, fm, s_buf,
           zrs, zrr, zls, zlr, bs, br, axs, axr, ays, ayr, fys, fyr, ads, adr, rss, rsr, os_, or_):
    d = lax.axis_index("depth")
    y = lax.axis_index("row")
    z = lax.axis_index("col")
    x = d // 2
    c = lax.rem(d, 2)
    ra = a_in.shape[0]
    rb = b_in.shape[0]
    kx = a_in.shape[1] // X
    nd = b_in.shape[1] // (2 * Y)
    nb = nd // NC

    def rel(v, k, n):
        return lax.rem(v + k + n, n)

    def dev(dx=0, cx=0, dy=0, dz=0):
        cc = c if cx == 0 else 1 - c
        xx = x if dx == 0 else rel(x, dx, X)
        yy = y if isinstance(dy, int) and dy == 0 else rel(y, dy, Y)
        zz = z if dz == 0 else rel(z, dz, Z)
        return {"depth": 2 * xx + cc, "row": yy, "col": zz}

    def remote(src, dst, ss, rs, device):
        return pltpu.make_async_remote_copy(
            src_ref=src, dst_ref=dst, send_sem=ss, recv_sem=rs,
            device_id=device, device_id_type=pl.DeviceIdType.MESH)

    def zr(t):
        j, i = t // STEPS, lax.rem(t, STEPS)
        sh = rel(z, -(i // 2), Z)
        s = lax.rem(i, 2)
        ref = b_buf.at[j, pl.ds(4 * s, 4), pl.ds(pl.multiple_of(sh * rb, rb), rb), :]
        return remote(ref, ref, zrs.at[j, i], zrr.at[j, i], dev(dz=1))

    def zl(t):
        j, i = t // STEPS, lax.rem(t, STEPS)
        sh = rel(z, i // 2, Z)
        s = 1 - lax.rem(i, 2)
        ref = b_buf.at[j, pl.ds(4 * s, 4), pl.ds(pl.multiple_of(sh * rb, rb), rb), :]
        return remote(ref, ref, zls.at[j, i], zlr.at[j, i], dev(dz=-1))

    def bpiece(j, cx, dy):
        yy = rel(y, dy, Y)
        cc = c if cx == 0 else 1 - c
        src = b_in.at[:, pl.ds(pl.multiple_of((yy * 2 + cc) * nd + j * nb, nb), nb)]
        dst = b_buf.at[j, c * Y + y, pl.ds(pl.multiple_of(z * rb, rb), rb), :]
        m = cx * Y + dy
        if m == 0:
            return pltpu.make_async_copy(src, dst, br.at[j, 0])
        return remote(src, dst, bs.at[j, m], br.at[j, m], dev(cx=cx, dy=dy))

    BP = [(cx, dy) for dy in (2, 1, 3, 0) for cx in (0, 1)]

    def bstart(j):
        for cx, dy in BP:
            bpiece(j, cx, dy).start()

    def bwait(j):
        for cx, dy in BP:
            p = bpiece(j, cx, dy)
            if (cx, dy) == (0, 0):
                p.wait()
            else:
                p.wait_recv()

    def aslot(yr, k, cc):
        yy = rel(y, yr, Y)
        dd = 2 * rel(x, -k, X) + cc
        return a_buf.at[yy, pl.ds(pl.multiple_of(dd * ra, ra), ra), :]

    def acols(xx):
        return a_in.at[:, pl.ds(pl.multiple_of(xx * kx, kx), kx)]

    def ax(k):
        return remote(acols(rel(x, k, X)), aslot(0, 0, c), axs.at[k], axr.at[k], dev(dx=k))

    def asrc(yr, k):
        if yr == 0 and k == 0:
            return acols(x)
        return aslot(yr, k, c)

    def ay(up, k):
        return remote(asrc(0, k), aslot(0, k, c), ays.at[up, k], ayr.at[up, k], dev(dy=1 if up else -1))

    def fy(up, k):
        ref = aslot(-1 if up else 1, k, c)
        return remote(ref, ref, fys.at[up, k], fyr.at[up, k], dev(dy=1 if up else -1))

    def ad(yr, k):
        return remote(asrc(yr, k), aslot(yr, k, c), ads.at[yr, k], adr.at[yr, k], dev(cx=1))

    def aown():
        return pltpu.make_async_copy(acols(x), aslot(0, 0, c), axr.at[0])

    def crow(q, dx, cc):
        dd = 2 * rel(x, dx, X) + cc
        return c_buf.at[q, pl.ds(pl.multiple_of(dd * ra, ra), ra), :]

    def rs(q, m):
        up = m % 2 == 0
        src = (crow(q, 2, 0), crow(q, 2, 1), crow(q, 1, 1), crow(q, -1, 0), crow(q, 1, 0), crow(q, -1, 1))[m]
        dst = (rp.at[q], rm.at[q], fp.at[q, 1], fm.at[q, 0], fp.at[q, 0], fm.at[q, 1])[m]
        return remote(src, dst, rss.at[q, m], rsr.at[q, m], dev(dx=1 if up else -1))

    def ocopy(q, cx, own):
        j, yr = q // Y, lax.rem(q, Y)
        cc = c if cx == 0 else 1 - c
        dst = out.at[:, pl.ds(pl.multiple_of((2 * y + c) * nd + j * nb, nb), nb)]
        src = s_buf.at[q, cx]
        if own:
            return pltpu.make_async_copy(src, dst, os_.at[q, cx])
        return remote(src, dst, os_.at[q, cx], or_.at[q, cx], {"depth": 2 * x + cc, "row": rel(y, yr, Y), "col": z})

    peers = [dict(dx=1), dict(dx=2), dict(dx=3), dict(dz=1), dict(dz=-1)]
    peers += [dict(cx=cx, dy=dy) for cx, dy in BP if (cx, dy) != (0, 0)]
    barrier = pltpu.get_barrier_semaphore()
    for p in peers:
        pl.semaphore_signal(barrier, inc=1, device_id=dev(**p), device_id_type=pl.DeviceIdType.MESH)
    pl.semaphore_wait(barrier, len(peers))

    bstart(0)
    ax(1).start()
    ax(3).start()
    ax(2).start()
    ay(1, 0).start()
    ay(0, 0).start()
    ad(0, 0).start()
    aown().start()

    def ev_x(k):
        ax(k).wait_recv()
        ay(1, k).start()
        ay(0, k).start()
        ad(0, k).start()

    def ev_y(k):
        ay(1, k).wait_recv()
        ay(0, k).wait_recv()
        up = 1 if k in (0, 2) else 0
        fy(up, k).start()
        ad(3, k).start()
        ad(1, k).start()

    def ev_f(k):
        fy(1 if k in (0, 2) else 0, k).wait_recv()
        ad(2, k).start()

    def ev_all():
        aown().wait()
        for yr in range(Y):
            for k in range(X):
                ad(yr, k).wait_recv()

    events = [(3, ev_x, 1), (3, ev_x, 3), (6, ev_y, 0), (8, ev_x, 2), (10, ev_y, 1), (14, ev_y, 3),
              (17, ev_y, 2), (20, ev_f, 0), (20, ev_f, 1), (23, ev_f, 3), (23, ev_f, 2), (FIRST, ev_all, None)]

    def tick(t, carry):
        i = lax.rem(t, STEPS)

        @pl.when(jnp.logical_and(t >= 2, t < NC * STEPS + 2))
        def _():
            zr(t - 2).wait_recv()
            zl(t - 2).wait_recv()

        @pl.when(t < NC * STEPS)
        def _():
            @pl.when(i == 0)
            def _():
                bwait(t // STEPS)

            zr(t).start()
            zl(t).start()

            @pl.when(jnp.logical_and(i == 1, t < (NC - 1) * STEPS))
            def _():
                bstart(t // STEPS + 1)

        for when, fn, arg in events:
            @pl.when(t == when)
            def _():
                fn() if arg is None else fn(arg)

        def stage(lag, fn):
            q = t - FIRST - lag

            @pl.when(jnp.logical_and(q >= 0, q < TILES))
            def _():
                fn(q)

        def s1(q):
            for m in range(4):
                rs(q, m).start()

        def s2(q):
            rs(q, 0).wait_recv()
            rs(q, 1).wait_recv()
            u, v = crow(q, 1, 0), crow(q, -1, 1)
            u[...] = u[...] + rp[q]
            v[...] = v[...] + rm[q]

        def s2b(q):
            rs(q, 4).start()
            rs(q, 5).start()

        def s3(q):
            for m in range(2, 6):
                rs(q, m).wait_recv()
            for cx in range(2):
                cc = c if cx == 0 else 1 - c
                total = crow(q, 0, cc)[...] + fp[q, cc] + fm[q, cc]
                s_buf[q, cx] = total.astype(s_buf.dtype)

        def s4(q):
            ocopy(q, 1, False).start()

            @pl.when(lax.rem(q, Y) == 0)
            def _():
                ocopy(q, 0, True).start()

            @pl.when(lax.rem(q, Y) != 0)
            def _():
                ocopy(q, 0, False).start()

        def tile(q):
            j, yy = q // Y, rel(y, lax.rem(q, Y), Y)
            kb = b_buf.shape[2]

            def part(k):
                return jnp.dot(a_buf[yy, :, pl.ds(pl.multiple_of(k * kb, kb), kb)], b_buf[j, k],
                               preferred_element_type=jnp.float32)

            c_buf[q] = part(0)

            def add(k, carry):
                c_buf[q] = c_buf[q] + part(k)
                return carry

            lax.fori_loop(1, b_buf.shape[1], add, None)

        stage(1, s1)
        stage(4, s2b)
        stage(3, s2)
        stage(8, s4)
        stage(7, s3)
        stage(0, tile)
        return carry

    lax.fori_loop(0, FIRST + TILES + 8, tick, None)

    def zdone(t, carry):
        zr(t).wait_send()
        zl(t).wait_send()
        return carry

    lax.fori_loop(0, NC * STEPS, zdone, None)

    def bdone(j, carry):
        for cx, dy in BP:
            if (cx, dy) != (0, 0):
                bpiece(j, cx, dy).wait_send()
        return carry

    lax.fori_loop(0, NC, bdone, None)
    for k in range(X):
        if k:
            ax(k).wait_send()
        ay(1, k).wait_send()
        ay(0, k).wait_send()
        fy(1 if k in (0, 2) else 0, k).wait_send()
        for yr in range(Y):
            ad(yr, k).wait_send()

    def qdone(q, carry):
        for m in range(6):
            rs(q, m).wait_send()
        far = ocopy(q, 1, False)
        far.wait_send()
        far.wait_recv()

        @pl.when(lax.rem(q, Y) == 0)
        def _():
            ocopy(q, 0, True).wait()

        @pl.when(lax.rem(q, Y) != 0)
        def _():
            near = ocopy(q, 0, False)
            near.wait_send()
            near.wait_recv()

        return carry

    lax.fori_loop(0, TILES, qdone, None)


def solution(mesh):
    all_axes = ("depth", "row", "col")

    def device_block(a_rows, b_rows):
        ra, k = a_rows.shape
        rb, n = b_rows.shape
        nb = n // (2 * Y) // NC
        dma = pltpu.SemaphoreType.DMA
        f32, bf16 = jnp.float32, a_rows.dtype
        scratch = [
            pltpu.VMEM((Y, 2 * X * ra, k // X), bf16),
            pltpu.VMEM((NC, 2 * Y, Z * rb, nb), bf16),
            pltpu.VMEM((TILES, 2 * X * ra, nb), f32),
            pltpu.VMEM((TILES, ra, nb), f32),
            pltpu.VMEM((TILES, ra, nb), f32),
            pltpu.VMEM((TILES, 2, ra, nb), f32),
            pltpu.VMEM((TILES, 2, ra, nb), f32),
            pltpu.VMEM((TILES, 2, ra, nb), bf16),
            dma((NC, STEPS)), dma((NC, STEPS)), dma((NC, STEPS)), dma((NC, STEPS)),
            dma((NC, 2 * Y)), dma((NC, 2 * Y)),
            dma((X,)), dma((X,)), dma((2, X)), dma((2, X)), dma((2, X)), dma((2, X)),
            dma((Y, X)), dma((Y, X)),
            dma((TILES, 6)), dma((TILES, 6)), dma((TILES, 2)), dma((TILES, 2)),
        ]
        return pl.pallas_call(
            kernel,
            out_shape=jax.ShapeDtypeStruct((ra, n), bf16),
            in_specs=[pl.BlockSpec(memory_space=pl.ANY)] * 2,
            out_specs=pl.BlockSpec(memory_space=pl.ANY),
            scratch_shapes=scratch,
            compiler_params=pltpu.CompilerParams(
                collective_id=0, has_side_effects=True, vmem_limit_bytes=67043328),
        )(a_rows, b_rows)

    return jax.shard_map(device_block, mesh=mesh, in_specs=(P(all_axes, None), P(all_axes, None)),
                         out_specs=P(all_axes, None), check_vma=False)
```

```python
import jax
import jax.numpy as jnp
from jax import lax
from jax.experimental import pallas as pl
from jax.experimental.pallas import tpu as pltpu
from jax.sharding import PartitionSpec as P

X = 4
Y = 4
Z = 8
BLOCKS = 12
PAIRS = 5
LEAD = 5
RING = LEAD + 8 * (BLOCKS // 2) + 4
FIRST = 34
PT = PAIRS * Y
ST = (BLOCKS - 2 * PAIRS) * Y


def kernel(a_in, b_in, out, a_buf, b_buf, c2, c1, rp2, rp1, rm2, rm1, fp2, fp1, fm2, fm1, s2_, s1_,
           pps, ppr, pms, pmr, zps, zpr, zms, zmr, bs, br, axs, axr, ays, ayr, fys, fyr, ads, adr,
           rss2, rsr2, rss1, rsr1, os2, or2, os1, or1):
    d = lax.axis_index("depth")
    y = lax.axis_index("row")
    z = lax.axis_index("col")
    x = d // 2
    c = lax.rem(d, 2)
    ra = a_in.shape[0]
    rb = b_in.shape[0]
    kx = a_in.shape[1] // X
    nd = b_in.shape[1] // (2 * Y)
    nb = nd // BLOCKS
    kb = Z * rb

    def rel(v, k, n):
        return lax.rem(v + k + n, n)

    def core(cx):
        return c if cx == 0 else 1 - c

    def dev(dx=0, cx=0, dy=0, dz=0):
        xx = x if isinstance(dx, int) and dx == 0 else rel(x, dx, X)
        yy = y if isinstance(dy, int) and dy == 0 else rel(y, dy, Y)
        zz = z if isinstance(dz, int) and dz == 0 else rel(z, dz, Z)
        return {"depth": 2 * xx + core(cx), "row": yy, "col": zz}

    def remote(src, dst, ss, rs, device):
        return pltpu.make_async_remote_copy(
            src_ref=src, dst_ref=dst, send_sem=ss, recv_sem=rs,
            device_id=device, device_id_type=pl.DeviceIdType.MESH)

    def own_msg(up, i):
        s = lax.rem(i, 2) if up else 1 - lax.rem(i, 2)
        sh = rel(z, -(i // 2) if up else i // 2, Z)
        half = BLOCKS // 2
        ref = b_buf.at[pl.ds(half * s, half), 0, pl.ds(pl.multiple_of(sh * rb, rb), rb), :]
        ss, rs = (pps, ppr) if up else (pms, pmr)
        return remote(ref, ref, ss.at[i], rs.at[i], dev(dz=1 if up else -1))

    def block_msg(up, blk, h, half):
        sh = rel(z, -h if up else h, Z)
        if half:
            n = rb // 2
            off = sh * rb + (0 if up else n)
        else:
            n, off = rb, sh * rb
        ref = b_buf.at[blk, pl.ds(1, 2 * Y - 1), pl.ds(pl.multiple_of(off, n), n), :]
        ss, rs = (zps, zpr) if up else (zms, zmr)
        return remote(ref, ref, ss.at[blk, h], rs.at[blk, h], dev(dz=1 if up else -1))

    def ring(t, act):
        v = t + (8 - LEAD)
        per, p = v // 8 - 1, lax.rem(v, 8)
        blk = 2 * per + lax.rem(p, 2) * (2 * (p // 4) - 1)
        h = lax.rem(p // 2 + 2 * lax.rem(p, 2), 4)
        block = jnp.logical_and(t >= LEAD, jnp.logical_and(blk >= 0, blk < BLOCKS))

        @pl.when(jnp.logical_and(t >= 0, t < LEAD))
        def _():
            for up in (True, False):
                act(own_msg(up, t))

        @pl.when(jnp.logical_and(t >= LEAD, blk < 0))
        def _():
            for up in (True, False):
                act(own_msg(up, LEAD + p // 2))

        @pl.when(jnp.logical_and(block, h < 3))
        def _():
            for up in (True, False):
                act(block_msg(up, blk, h, False))

        @pl.when(jnp.logical_and(block, h == 3))
        def _():
            for up in (True, False):
                act(block_msg(up, blk, h, True))

        return block, blk, h

    BP = [(cx, dy) for dy in (2, 1, 3, 0) for cx in (0, 1) if (cx, dy) != (0, 0)]

    def bcols(cx, dy, blk):
        yy = rel(y, dy, Y)
        return b_in.at[:, pl.ds(pl.multiple_of((yy * 2 + core(cx)) * nd + blk * nb, nb), nb)]

    def bpiece(blk, cx, dy):
        m = cx * Y + (Y - dy) % Y
        dst = b_buf.at[blk, m, pl.ds(pl.multiple_of(z * rb, rb), rb), :]
        return remote(bcols(cx, dy, blk), dst, bs.at[blk, m], br.at[blk, m], dev(cx=cx, dy=dy))

    def bown(blk):
        return pltpu.make_async_copy(
            bcols(0, 0, blk), b_buf.at[blk, 0, pl.ds(pl.multiple_of(z * rb, rb), rb), :], br.at[blk, 0])

    def bstart(blk):
        for cx, dy in BP:
            bpiece(blk, cx, dy).start()

    def bwait(blk):
        for cx, dy in BP:
            bpiece(blk, cx, dy).wait_recv()

    def aslot(yr, k, cc):
        dd = 2 * rel(x, -k, X) + cc
        return a_buf.at[rel(y, yr, Y), pl.ds(pl.multiple_of(dd * ra, ra), ra), :]

    def acols(xx):
        return a_in.at[:, pl.ds(pl.multiple_of(xx * kx, kx), kx)]

    def ax(k):
        return remote(acols(rel(x, k, X)), aslot(0, 0, c), axs.at[k], axr.at[k], dev(dx=k))

    def asrc(yr, k):
        if yr == 0 and k == 0:
            return acols(x)
        return aslot(yr, k, c)

    def ay(up, k):
        return remote(asrc(0, k), aslot(0, k, c), ays.at[up, k], ayr.at[up, k], dev(dy=1 if up else -1))

    def fy(k):
        up = k in (0, 2)
        ref = aslot(-1 if up else 1, k, c)
        return remote(ref, ref, fys.at[k], fyr.at[k], dev(dy=1 if up else -1))

    def ad(yr, k):
        return remote(asrc(yr, k), aslot(yr, k, c), ads.at[yr, k], adr.at[yr, k], dev(cx=1))

    def aown():
        return pltpu.make_async_copy(acols(x), aslot(0, 0, c), axr.at[0])

    class Tiles:
        def __init__(self, c_, rp, rm, fp, fm, s_, rss, rsr, oss, osr, first, width):
            self.c, self.rp, self.rm, self.fp, self.fm, self.s = c_, rp, rm, fp, fm, s_
            self.rss, self.rsr, self.oss, self.osr = rss, rsr, oss, osr
            self.first, self.width = first, width

        def rows(self, q, dx, cc):
            dd = 2 * rel(x, dx, X) + cc
            return self.c.at[q, pl.ds(pl.multiple_of(dd * ra, ra), ra), :]

        def part(self, q, m):
            src = (self.rows(q, 2, 0), self.rows(q, 2, 1), self.rows(q, 1, 1),
                   self.rows(q, -1, 0), self.rows(q, 1, 0), self.rows(q, -1, 1))[m]
            dst = (self.rp.at[q], self.rm.at[q], self.fp.at[q, 1],
                   self.fm.at[q, 0], self.fp.at[q, 0], self.fm.at[q, 1])[m]
            return remote(src, dst, self.rss.at[q, m], self.rsr.at[q, m], dev(dx=1 if m % 2 == 0 else -1))

        def piece(self, q, cx, own=False):
            n = nb * self.width
            col = (2 * y + c) * nd + (self.first + (q // Y) * self.width) * nb
            dst = out.at[:, pl.ds(pl.multiple_of(col, nb), n)]
            if own:
                return pltpu.make_async_copy(self.s.at[q, cx], dst, self.oss.at[q, cx])
            return remote(self.s.at[q, cx], dst, self.oss.at[q, cx], self.osr.at[q, cx],
                          dev(cx=cx, dy=lax.rem(q, Y)))

        def tile(self, q):
            blk = self.first + (q // Y) * self.width
            yy = rel(y, lax.rem(q, Y), Y)
            total = None
            for m in range(2 * Y):
                src = core(m // Y) * Y + rel(y, m % Y, Y)
                lhs = a_buf[yy, :, pl.ds(pl.multiple_of(src * kb, kb), kb)]
                rhs = [b_buf[blk + i, m] for i in range(self.width)]
                rhs = rhs[0] if self.width == 1 else jnp.concatenate(rhs, axis=1)
                part = jnp.dot(lhs, rhs, preferred_element_type=jnp.float32)
                total = part if total is None else total + part
            self.c[q] = total

        def send(self, q):
            for m in range(4):
                self.part(q, m).start()

        def relay(self, q):
            self.part(q, 0).wait_recv()
            self.part(q, 1).wait_recv()
            u, v = self.rows(q, 1, 0), self.rows(q, -1, 1)
            u[...] = u[...] + self.rp[q]
            v[...] = v[...] + self.rm[q]

        def send_relayed(self, q):
            self.part(q, 4).start()
            self.part(q, 5).start()

        def finish(self, q):
            for m in range(2, 6):
                self.part(q, m).wait_recv()
            for cx in range(2):
                cc = core(cx)
                total = self.rows(q, 0, cc)[...] + self.fp[q, cc] + self.fm[q, cc]
                self.s[q, cx] = total.astype(self.s.dtype)

        def output(self, q):
            self.piece(q, 1).start()

            @pl.when(lax.rem(q, Y) == 0)
            def _():
                self.piece(q, 0, True).start()

            @pl.when(lax.rem(q, Y) != 0)
            def _():
                self.piece(q, 0).start()

        def sent(self, q):
            for m in range(6):
                self.part(q, m).wait_send()

        def done(self, q):
            far = self.piece(q, 1)
            far.wait_send()
            far.wait_recv()

            @pl.when(lax.rem(q, Y) == 0)
            def _():
                self.piece(q, 0, True).wait()

            @pl.when(lax.rem(q, Y) != 0)
            def _():
                near = self.piece(q, 0)
                near.wait_send()
                near.wait_recv()

    two = Tiles(c2, rp2, rm2, fp2, fm2, s2_, rss2, rsr2, os2, or2, 0, 2)
    one = Tiles(c1, rp1, rm1, fp1, fm1, s1_, rss1, rsr1, os1, or1, 2 * PAIRS, 1)

    for blk in range(BLOCKS):
        bown(blk).start()
    aown().start()

    peers = [dict(dx=1), dict(dx=2), dict(dx=3), dict(dz=1), dict(dz=-1)]
    peers += [dict(cx=cx, dy=dy) for cx, dy in BP]
    barrier = pltpu.get_barrier_semaphore()
    for p in peers:
        pl.semaphore_signal(barrier, inc=1, device_id=dev(**p), device_id_type=pl.DeviceIdType.MESH)
    for blk in range(BLOCKS):
        bown(blk).wait()
    pl.semaphore_wait(barrier, len(peers))

    def a_first():
        ax(1).start()
        ax(3).start()
        ax(2).start()
        bstart(0)
        bstart(1)
        ay(1, 0).start()
        ay(0, 0).start()
        ad(0, 0).start()

    def a_x(k):
        ax(k).wait_recv()
        ay(1, k).start()
        ay(0, k).start()
        ad(0, k).start()

    def a_y(k):
        ay(1, k).wait_recv()
        ay(0, k).wait_recv()
        fy(k).start()
        ad(3, k).start()
        ad(1, k).start()

    def a_f(k):
        fy(k).wait_recv()
        ad(2, k).start()

    def a_all():
        aown().wait()
        for yr in range(Y):
            for k in range(X):
                ad(yr, k).wait_recv()

    def a_sent():
        for k in range(X):
            if k:
                ax(k).wait_send()
            ay(1, k).wait_send()
            ay(0, k).wait_send()
            fy(k).wait_send()
            for yr in range(Y):
                ad(yr, k).wait_send()

    def b_sent():
        def body(blk, carry):
            for cx, dy in BP:
                bpiece(blk, cx, dy).wait_send()
            return carry

        lax.fori_loop(0, BLOCKS, body, None)

    events = [(0, a_first, ()), (5, a_x, (1,)), (5, a_x, (3,)), (12, a_x, (2,)), (13, a_y, (0,)), (13, a_y, (1,)),
              (17, a_y, (3,)), (21, a_y, (2,)), (31, a_f, (0,)), (31, a_f, (1,)), (33, a_f, (3,)), (33, a_f, (2,)),
              (FIRST, a_all, ()), (42, a_sent, ()), (46, b_sent, ())]

    def tick(t, carry):
        ring(t - 2, lambda m: m.wait_recv())
        v = t + (8 - LEAD)
        per, p = v // 8 - 1, lax.rem(v, 8)
        live = jnp.logical_and(t >= LEAD, per < BLOCKS // 2)

        @pl.when(jnp.logical_and(live, p == 0))
        def _():
            bwait(2 * per)

        @pl.when(jnp.logical_and(live, p == 5))
        def _():
            bwait(2 * per + 1)

        ring(t, lambda m: m.start())

        @pl.when(jnp.logical_and(p == 7, per < BLOCKS // 2 - 2))
        def _():
            bstart(2 * per + 4)
            bstart(2 * per + 5)

        for when, fn, arg in events:
            @pl.when(t == when)
            def _():
                fn(*arg)

        ring(t - 8, lambda m: m.wait_send())

        def stage(lag, name):
            u = t - FIRST - lag

            @pl.when(jnp.logical_and(u >= 0, u < PT))
            def _():
                getattr(two, name)(u)

            @pl.when(jnp.logical_and(u >= PT, u < PT + ST))
            def _():
                getattr(one, name)(u - PT)

        stage(1, "send")
        stage(4, "send_relayed")
        stage(7, "output")
        stage(3, "relay")
        stage(6, "finish")
        stage(0, "tile")
        stage(9, "sent")
        stage(10, "done")
        return carry

    lax.fori_loop(0, FIRST + PT + ST + 10, tick, None)


def solution(mesh):
    all_axes = ("depth", "row", "col")

    def device_block(a_rows, b_rows):
        ra, k = a_rows.shape
        rb, n = b_rows.shape
        nb = n // (2 * Y) // BLOCKS
        dma = pltpu.SemaphoreType.DMA
        f32, bf16 = jnp.float32, a_rows.dtype

        def both(*tail, dtype):
            return [pltpu.VMEM((PT, *tail, 2 * nb), dtype), pltpu.VMEM((ST, *tail, nb), dtype)]

        scratch = [
            pltpu.VMEM((Y, 2 * X * ra, k // X), bf16),
            pltpu.VMEM((BLOCKS, 2 * Y, Z * rb, nb), bf16),
            *both(2 * X * ra, dtype=f32),
            *both(ra, dtype=f32), *both(ra, dtype=f32),
            *both(2, ra, dtype=f32), *both(2, ra, dtype=f32),
            *both(2, ra, dtype=bf16),
            dma((7,)), dma((7,)), dma((7,)), dma((7,)),
            dma((BLOCKS, 4)), dma((BLOCKS, 4)), dma((BLOCKS, 4)), dma((BLOCKS, 4)),
            dma((BLOCKS, 2 * Y)), dma((BLOCKS, 2 * Y)),
            dma((X,)), dma((X,)), dma((2, X)), dma((2, X)), dma((X,)), dma((X,)),
            dma((Y, X)), dma((Y, X)),
            dma((PT, 6)), dma((PT, 6)), dma((ST, 6)), dma((ST, 6)),
            dma((PT, 2)), dma((PT, 2)), dma((ST, 2)), dma((ST, 2)),
        ]
        return pl.pallas_call(
            kernel,
            out_shape=jax.ShapeDtypeStruct((ra, n), bf16),
            in_specs=[pl.BlockSpec(memory_space=pl.ANY)] * 2,
            out_specs=pl.BlockSpec(memory_space=pl.ANY),
            scratch_shapes=scratch,
            compiler_params=pltpu.CompilerParams(
                collective_id=0, has_side_effects=True, vmem_limit_bytes=67043328),
        )(a_rows, b_rows)

    return jax.shard_map(device_block, mesh=mesh, in_specs=(P(all_axes, None), P(all_axes, None)),
                         out_specs=P(all_axes, None), check_vma=False)
```

```python
import jax
import jax.numpy as jnp
from jax import lax
from jax.experimental import pallas as pl
from jax.experimental.pallas import tpu as pltpu
from jax.sharding import PartitionSpec as P

X = 4
Y = 4
Z = 8
BLOCKS = 12
PAIRS = 4
LEAD = 6
END = 43
FIRST = 21
SINGLE = 34
PT = PAIRS * Y
ST = (BLOCKS - 2 * PAIRS) * Y


def kernel(a_in, b_in, out, a_buf, b_buf, c2, c1, rp2, rp1, rm2, rm1, fp2, fp1, fm2, fm1, s2_, s1_,
           zps, zpr, zms, zmr, bs, br, bo, axr, ayr, fyr, adr, as24, as7,
           rss2, rsr2, rsf2, oss2, osr2, oso2, rss1, rsr1, rsf1, oss1, osr1, oso1):
    d = lax.axis_index("depth")
    y = lax.axis_index("row")
    z = lax.axis_index("col")
    x = d // 2
    c = lax.rem(d, 2)
    ra = a_in.shape[0]
    rb = b_in.shape[0]
    kx = a_in.shape[1] // X
    nd = b_in.shape[1] // (2 * Y)
    nb = nd // BLOCKS
    kb = Z * rb

    def rel(v, k, n):
        return lax.rem(v + k + n, n)

    def core(cx):
        return c if cx == 0 else 1 - c

    def dev(dx=0, cx=0, dy=0, dz=0):
        xx = x if isinstance(dx, int) and dx == 0 else rel(x, dx, X)
        yy = y if isinstance(dy, int) and dy == 0 else rel(y, dy, Y)
        zz = z if isinstance(dz, int) and dz == 0 else rel(z, dz, Z)
        return {"depth": 2 * xx + core(cx), "row": yy, "col": zz}

    def remote(src, dst, ss, rs, device):
        return pltpu.make_async_remote_copy(
            src_ref=src, dst_ref=dst, send_sem=ss, recv_sem=rs,
            device_id=device, device_id_type=pl.DeviceIdType.MESH)

    def landed(ref, sem):
        remote(ref, ref, bs, sem, dev(dz=1)).wait_recv()

    def left(ref, sem):
        remote(ref, ref, sem, bo, dev(dz=1)).wait_send()

    def sems(up, kind, t):
        ss, rs = (zps, zpr) if up else (zms, zmr)
        return ss.at[kind, lax.rem(t, 4)], rs.at[kind, lax.rem(t, 4)]

    def own_msg(up, i, t):
        s = lax.rem(i, 2) if up else 1 - lax.rem(i, 2)
        sh = rel(z, -(i // 2) if up else i // 2, Z)
        half = BLOCKS // 2
        ref = b_buf.at[pl.ds(half * s, half), 0, pl.ds(pl.multiple_of(sh * rb, rb), rb), :]
        return remote(ref, ref, *sems(up, 0, t), dev(dz=1 if up else -1))

    def block_msg(up, blk, h, half, t):
        sh = rel(z, -h if up else h, Z)
        if half:
            n = rb // 2
            off = sh * rb + (0 if up else n)
        else:
            n, off = rb, sh * rb
        ref = b_buf.at[blk, pl.ds(1, 2 * Y - 1), pl.ds(pl.multiple_of(off, n), n), :]
        return remote(ref, ref, *sems(up, 1 if half else 0, t), dev(dz=1 if up else -1))

    def last_msg(up, h, i):
        sh = rel(z, -h if up else h, Z)
        n = rb // 2
        off = sh * rb + n * (i if up else 1 - i)
        ref = b_buf.at[BLOCKS - 1, pl.ds(1, 2 * Y - 1), pl.ds(pl.multiple_of(off, n), n), :]
        return remote(ref, ref, *sems(up, i, END - 4 + 2 * h), dev(dz=1 if up else -1))

    def ring(t, act):
        u = t - LEAD
        odd = lax.rem(u, 2)
        k = (u + 3 * odd) // 2
        blk, h = 2 * (k // 3) - odd, lax.rem(k, 3)
        block = (t >= LEAD) & (blk >= 0)

        @pl.when((t >= 0) & ((t < LEAD) | (blk < 0)))
        def _():
            for up in (True, False):
                act(own_msg(up, t - t // (LEAD + 1), t))

        @pl.when(block & (h == 0) & (blk >= 2))
        def _():
            for up in (True, False):
                act(block_msg(up, blk - 2, 3, True, t))

        @pl.when(block & (3 * blk + h <= 3 * (BLOCKS - 1)))
        def _():
            for up in (True, False):
                act(block_msg(up, blk, h, False, t))

    BP = [(cx, dy) for dy in (2, 1, 3, 0) for cx in (0, 1) if (cx, dy) != (0, 0)]

    def bcols(cx, dy, blk):
        yy = rel(y, dy, Y)
        return b_in.at[:, pl.ds(pl.multiple_of((yy * 2 + core(cx)) * nd + blk * nb, nb), nb)]

    def bpiece(blk, cx, dy):
        m = cx * Y + (Y - dy) % Y
        dst = b_buf.at[blk, m, pl.ds(pl.multiple_of(z * rb, rb), rb), :]
        return remote(bcols(cx, dy, blk), dst, bs, br.at[blk], dev(cx=cx, dy=dy))

    def bown(blk):
        return pltpu.make_async_copy(
            bcols(0, 0, blk), b_buf.at[blk, 0, pl.ds(pl.multiple_of(z * rb, rb), rb), :], bo)

    def bstart(blk):
        for cx, dy in BP:
            bpiece(blk, cx, dy).start()

    def bwait(blk):
        landed(b_buf.at[blk, pl.ds(1, 2 * Y - 1), pl.ds(pl.multiple_of(z * rb, rb), rb), :], br.at[blk])

    def aslot(yr, k, cc):
        dd = 2 * rel(x, -k, X) + cc
        return a_buf.at[rel(y, yr, Y), pl.ds(pl.multiple_of(dd * ra, ra), ra), :]

    def acols(xx):
        return a_in.at[:, pl.ds(pl.multiple_of(xx * kx, kx), kx)]

    def ax(k):
        return remote(acols(rel(x, k, X)), aslot(0, 0, c), as7, axr.at[k], dev(dx=k))

    def asrc(yr, k):
        if yr == 0 and k == 0:
            return acols(x)
        return aslot(yr, k, c)

    def ay(up, k):
        return remote(asrc(0, k), aslot(0, k, c), as24, ayr.at[up, k], dev(dy=1 if up else -1))

    def fy(k):
        up = k in (0, 2)
        ref = aslot(-1 if up else 1, k, c)
        return remote(ref, ref, as7, fyr.at[k], dev(dy=1 if up else -1))

    def ad(yr, k):
        return remote(asrc(yr, k), aslot(yr, k, c), as24, adr.at[yr], dev(cx=1))

    def aown():
        return pltpu.make_async_copy(acols(x), aslot(0, 0, c), axr.at[0])

    class Tiles:
        def __init__(self, c_, rp, rm, fp, fm, s_, rss, rsr, rsf, oss, osr, oso, first, width):
            self.c, self.rp, self.rm, self.fp, self.fm, self.s = c_, rp, rm, fp, fm, s_
            self.rss, self.rsr, self.rsf, self.oss, self.osr, self.oso = rss, rsr, rsf, oss, osr, oso
            self.first, self.width = first, width

        def rows(self, q, dx, cc):
            dd = 2 * rel(x, dx, X) + cc
            return self.c.at[q, pl.ds(pl.multiple_of(dd * ra, ra), ra), :]

        def part(self, q, m):
            src = (self.rows(q, 2, 0), self.rows(q, 2, 1), self.rows(q, 1, 1),
                   self.rows(q, -1, 0), self.rows(q, 1, 0), self.rows(q, -1, 1))[m]
            dst = (self.rp.at[q], self.rm.at[q], self.fp.at[q, 1],
                   self.fm.at[q, 0], self.fp.at[q, 0], self.fm.at[q, 1])[m]
            return remote(src, dst, self.rss, (self.rsr if m < 2 else self.rsf).at[q], dev(dx=1 if m % 2 == 0 else -1))

        def piece(self, q, cx, own=False):
            n = nb * self.width
            col = (2 * y + c) * nd + (self.first + (q // Y) * self.width) * nb
            dst = out.at[:, pl.ds(pl.multiple_of(col, nb), n)]
            if own:
                return pltpu.make_async_copy(self.s.at[q, cx], dst, self.oso)
            return remote(self.s.at[q, cx], dst, self.oss, self.osr, dev(cx=cx, dy=lax.rem(q, Y)))

        def tile(self, q):
            blk = self.first + (q // Y) * self.width
            yy = rel(y, lax.rem(q, Y), Y)
            total = None
            for m in range(2 * Y):
                src = core(m // Y) * Y + rel(y, m % Y, Y)
                lhs = a_buf[yy, :, pl.ds(pl.multiple_of(src * kb, kb), kb)]
                rhs = [b_buf[blk + i, m] for i in range(self.width)]
                rhs = rhs[0] if self.width == 1 else jnp.concatenate(rhs, axis=1)
                part = jnp.dot(lhs, rhs, preferred_element_type=jnp.float32)
                total = part if total is None else total + part
            self.c[q] = total

        def send(self, q):
            for m in range(4):
                self.part(q, m).start()

        def relay(self, q):
            landed(self.c.at[q, pl.ds(0, 2 * ra), :], self.rsr.at[q])
            u, v = self.rows(q, 1, 0), self.rows(q, -1, 1)
            u[...] = u[...] + self.rp[q]
            v[...] = v[...] + self.rm[q]

        def send_relayed(self, q):
            self.part(q, 4).start()
            self.part(q, 5).start()

        def finish(self, q):
            landed(self.c.at[q, pl.ds(0, 4 * ra), :], self.rsf.at[q])
            for cx in range(2):
                cc = core(cx)
                total = self.rows(q, 0, cc)[...] + self.fp[q, cc] + self.fm[q, cc]
                self.s[q, cx] = total.astype(self.s.dtype)

        def output(self, q):
            self.piece(q, 1).start()

            @pl.when(lax.rem(q, Y) == 0)
            def _():
                self.piece(q, 0, True).start()

            @pl.when(lax.rem(q, Y) != 0)
            def _():
                self.piece(q, 0).start()

        def end(self, tiles):
            left(self.c.at[pl.ds(0, tiles * 6 // (2 * X)), :, :], self.rss)
            left(self.s.at[pl.ds(0, tiles * 7 // 8)], self.oss)
            landed(self.s.at[pl.ds(0, tiles // 8)], self.oso)
            landed(self.s.at[pl.ds(0, tiles * 7 // 8)], self.osr)

    two = Tiles(c2, rp2, rm2, fp2, fm2, s2_, rss2, rsr2, rsf2, oss2, osr2, oso2, 0, 2)
    one = Tiles(c1, rp1, rm1, fp1, fm1, s1_, rss1, rsr1, rsf1, oss1, osr1, oso1, 2 * PAIRS, 1)

    for blk in range(BLOCKS):
        bown(blk).start()
    aown().start()

    peers = [dict(dx=1), dict(dx=2), dict(dx=3), dict(dz=1), dict(dz=-1)]
    peers += [dict(cx=cx, dy=dy) for cx, dy in BP]
    barrier = pltpu.get_barrier_semaphore()
    for p in peers:
        pl.semaphore_signal(barrier, inc=1, device_id=dev(**p), device_id_type=pl.DeviceIdType.MESH)
    landed(b_buf.at[:, 0, pl.ds(pl.multiple_of(z * rb, rb), rb), :], bo)
    pl.semaphore_wait(barrier, len(peers))

    def a_first():
        ax(1).start()
        ax(3).start()
        ax(2).start()
        bstart(0)
        bstart(1)
        ay(1, 0).start()
        ay(0, 0).start()
        ad(0, 0).start()

    def a_x(k):
        ax(k).wait_recv()
        ay(1, k).start()
        ay(0, k).start()
        ad(0, k).start()

    def a_y(k):
        ay(1, k).wait_recv()
        ay(0, k).wait_recv()
        fy(k).start()
        ad(3, k).start()
        ad(1, k).start()

    def a_f(k):
        fy(k).wait_recv()
        ad(2, k).start()

    def a_rows(yr):
        if yr == 0:
            aown().wait()
        landed(a_buf.at[0, pl.ds(0, X * ra), :], adr.at[yr])

    def start(m):
        m.start()

    def recv(m):
        m.wait_recv()

    def sent(m):
        m.wait_send()

    def last_hop(h, i, act):
        for up in (True, False):
            act(last_msg(up, h, i))

    def run(t, group):
        for at, calls in group.items():
            @pl.when(t == at)
            def _():
                for fn, *arg in calls:
                    fn(*arg)

    ahead = {0: [(a_first,)], 5: [(a_x, 1), (a_x, 3)], 12: [(a_x, 2), (a_y, 0), (a_y, 1)], 14: [(a_y, 3)],
             18: [(a_y, 2)]}
    beside = {FIRST: [(a_rows, 0), (a_rows, 1), (a_rows, 3)], 26: [(a_f, 0), (a_f, 1)], 29: [(a_f, 3), (a_f, 2)],
              FIRST + 10: [(a_rows, 2)]}
    tail = {44: [(last_hop, 1, 0, recv), (last_hop, 2, 0, start), (last_hop, 1, 1, recv), (last_hop, 2, 1, start)],
            47: [(last_hop, 2, 0, recv), (last_hop, 1, 0, sent), (last_hop, 3, 0, start)],
            50: [(last_hop, 2, 1, recv), (last_hop, 1, 1, sent)], 52: [(last_hop, 3, 0, recv)]}
    last_slot = SINGLE + 6 * (BLOCKS - 2 * PAIRS - 1) + Y - 1

    def pair_stage(slot, name, lag):
        w = slot - lag
        i, r = w // 4, lax.rem(w, 4)
        late, last = i // 5, i // 7
        q = (1 - late) * (Y * (i - 2 * (i // 4)) + r + r // 2) + (late - last) * (Y * r + 2) + last * (12 + r)
        some = (r < 3) & ((i < 2) | (i == 4) | (i == 5))

        @pl.when((w >= 0) & (w < 32) & (some | (i == 7)))
        def _():
            getattr(two, name)(q)

    def block_stage(slot, name, lag):
        v = slot - SINGLE - lag
        k, r = v // 6, lax.rem(v, 6)

        @pl.when((v >= 0) & (k < BLOCKS - 2 * PAIRS) & (r < Y))
        def _():
            getattr(one, name)(Y * k + r)

    def slots(slot, carry):
        @pl.when(slot < 32 + 16)
        def _():
            pair_stage(slot, "send", 1)
            pair_stage(slot, "send_relayed", 7)
            pair_stage(slot, "output", 15)
            pair_stage(slot, "relay", 6)
            pair_stage(slot, "finish", 14)
            pair_stage(slot, "tile", 0)

        @pl.when(slot >= SINGLE)
        def _():
            block_stage(slot, "send", 1)

            @pl.when((slot >= 44) & (slot <= 52))
            def _():
                run(slot, tail)

            block_stage(slot, "send_relayed", 5)
            block_stage(slot, "output", 10)
            block_stage(slot, "tile", 0)
            block_stage(slot, "relay", 4)
            block_stage(slot, "finish", 9)

        return carry

    def tick(t, carry):
        @pl.when(t < END + 2)
        def _():
            ring(t - 2, recv)
            ring(t - 4, sent)
            ahead3 = lax.rem(t, 3)

            @pl.when((ahead3 == 0) & (t >= LEAD) & (t < LEAD + 3 * BLOCKS))
            def _():
                bwait((t - LEAD) // 3)

            @pl.when(t < END)
            def _():
                ring(t, start)

            @pl.when(t == END - 2)
            def _():
                last_hop(1, 0, start)
                last_hop(1, 1, start)

            @pl.when((ahead3 == 1) & (t >= 4) & (t < 3 * BLOCKS - 2))
            def _():
                bstart((t + 2) // 3)

            @pl.when(t < FIRST)
            def _():
                run(t, ahead)

            @pl.when(t >= FIRST)
            def _():
                run(t, beside)

        @pl.when(t >= FIRST)
        def _():
            first = 2 * (t - FIRST)
            lax.fori_loop(first, first + 2, slots, None)

        return carry

    lax.fori_loop(0, FIRST + (last_slot + 10) // 2 + 1, tick, None)

    def ring_sent(t, carry):
        ring(t, sent)
        return carry

    lax.fori_loop(END - 1, END, ring_sent, None)
    for h, i in ((2, 0), (2, 1), (3, 0)):
        last_hop(h, i, sent)
    left(b_buf.at[:, pl.ds(1, 2 * Y - 1), pl.ds(0, rb), :], bs)
    left(a_buf.at[pl.ds(0, 3)], as24)
    left(a_buf.at[0, pl.ds(0, 7 * ra), :], as7)
    two.end(PT)
    one.end(ST)


def solution(mesh):
    all_axes = ("depth", "row", "col")

    def device_block(a_rows, b_rows):
        ra, k = a_rows.shape
        rb, n = b_rows.shape
        nb = n // (2 * Y) // BLOCKS
        dma = pltpu.SemaphoreType.DMA
        f32, bf16 = jnp.float32, a_rows.dtype

        def both(*tail, dtype):
            return [pltpu.VMEM((PT, *tail, 2 * nb), dtype), pltpu.VMEM((ST, *tail, nb), dtype)]

        scratch = [
            pltpu.VMEM((Y, 2 * X * ra, k // X), bf16),
            pltpu.VMEM((BLOCKS, 2 * Y, Z * rb, nb), bf16),
            *both(2 * X * ra, dtype=f32),
            *both(ra, dtype=f32), *both(ra, dtype=f32),
            *both(2, ra, dtype=f32), *both(2, ra, dtype=f32),
            *both(2, ra, dtype=bf16),
            dma((2, 4)), dma((2, 4)), dma((2, 4)), dma((2, 4)),
            dma, dma((BLOCKS,)), dma, dma((X,)), dma((2, X)), dma((X,)), dma((Y,)), dma, dma,
            dma, dma((PT,)), dma((PT,)), dma, dma, dma,
            dma, dma((ST,)), dma((ST,)), dma, dma, dma,
        ]
        return pl.pallas_call(
            kernel,
            out_shape=jax.ShapeDtypeStruct((ra, n), bf16),
            in_specs=[pl.BlockSpec(memory_space=pl.ANY)] * 2,
            out_specs=pl.BlockSpec(memory_space=pl.ANY),
            scratch_shapes=scratch,
            compiler_params=pltpu.CompilerParams(
                collective_id=0, has_side_effects=True, vmem_limit_bytes=67043328),
        )(a_rows, b_rows)

    return jax.shard_map(device_block, mesh=mesh, in_specs=(P(all_axes, None), P(all_axes, None)),
                         out_specs=P(all_axes, None), check_vma=False)
```

```python
import jax
import jax.numpy as jnp
from jax import lax
from jax.experimental import pallas as pl
from jax.experimental.pallas import tpu as pltpu
from jax.sharding import PartitionSpec as P

X = 4
Y = 4
Z = 8
BLOCKS = 12
PAIRS = 4
LEAD = 6
END = 43
FIRST = 22
SINGLE = 32
PT = PAIRS * Y
ST = (BLOCKS - 2 * PAIRS) * Y


def kernel(a_in, b_in, out, a_buf, b_buf, c2, c1, rp2, rp1, rm2, rm1, fp2, fp1, fm2, fm1, s2_, s1_,
           zps, zpr, zms, zmr, bs, br, bo, axr, ayr, fyr, adr, as24, as7,
           rss2, rsr2, rsf2, oss2, osr2, rss1, rsr1, rsf1, oss1, osr1):
    d = lax.axis_index("depth")
    y = lax.axis_index("row")
    z = lax.axis_index("col")
    x = d // 2
    c = lax.rem(d, 2)
    ra = a_in.shape[0]
    rb = b_in.shape[0]
    kx = a_in.shape[1] // X
    nd = b_in.shape[1] // (2 * Y)
    nb = nd // BLOCKS
    kb = Z * rb

    def rel(v, k, n):
        return lax.rem(v + k + n, n)

    def core(cx):
        return c if cx == 0 else 1 - c

    def dev(dx=0, cx=0, dy=0, dz=0):
        xx = x if isinstance(dx, int) and dx == 0 else rel(x, dx, X)
        yy = y if isinstance(dy, int) and dy == 0 else rel(y, dy, Y)
        zz = z if isinstance(dz, int) and dz == 0 else rel(z, dz, Z)
        return {"depth": 2 * xx + core(cx), "row": yy, "col": zz}

    def remote(src, dst, ss, rs, device):
        return pltpu.make_async_remote_copy(
            src_ref=src, dst_ref=dst, send_sem=ss, recv_sem=rs,
            device_id=device, device_id_type=pl.DeviceIdType.MESH)

    def landed(ref, sem):
        remote(ref, ref, bs, sem, dev(dz=1)).wait_recv()

    def left(ref, sem):
        remote(ref, ref, sem, bo, dev(dz=1)).wait_send()

    def sems(up, kind, t):
        ss, rs = (zps, zpr) if up else (zms, zmr)
        return ss.at[kind, lax.rem(t, 4)], rs.at[kind, lax.rem(t, 4)]

    def own_msg(up, i, t):
        s = lax.rem(i, 2) if up else 1 - lax.rem(i, 2)
        sh = rel(z, -(i // 2) if up else i // 2, Z)
        half = BLOCKS // 2
        ref = b_buf.at[pl.ds(half * s, half), 0, pl.ds(pl.multiple_of(sh * rb, rb), rb), :]
        return remote(ref, ref, *sems(up, 0, t), dev(dz=1 if up else -1))

    def block_msg(up, blk, h, half, t):
        sh = rel(z, -h if up else h, Z)
        if half:
            n = rb // 2
            off = sh * rb + (0 if up else n)
        else:
            n, off = rb, sh * rb
        ref = b_buf.at[blk, pl.ds(1, 2 * Y - 1), pl.ds(pl.multiple_of(off, n), n), :]
        return remote(ref, ref, *sems(up, 1 if half else 0, t), dev(dz=1 if up else -1))

    def last_msg(up, h, i):
        sh = rel(z, -h if up else h, Z)
        n = rb // 2
        off = sh * rb + n * (i if up else 1 - i)
        ref = b_buf.at[BLOCKS - 1, pl.ds(1, 2 * Y - 1), pl.ds(pl.multiple_of(off, n), n), :]
        return remote(ref, ref, *sems(up, i, END - 4 + 2 * h), dev(dz=1 if up else -1))

    def ring(t, act):
        u = t - LEAD
        odd = lax.rem(u, 2)
        k = (u + 3 * odd) // 2
        blk, h = 2 * (k // 3) - odd, lax.rem(k, 3)
        block = (t >= LEAD) & (blk >= 0)

        @pl.when((t >= 0) & ((t < LEAD) | (blk < 0)))
        def _():
            for up in (True, False):
                act(own_msg(up, t - t // (LEAD + 1), t))

        @pl.when(block & (h == 0) & (blk >= 2))
        def _():
            for up in (True, False):
                act(block_msg(up, blk - 2, 3, True, t))

        @pl.when(block & (3 * blk + h <= 3 * (BLOCKS - 1)))
        def _():
            for up in (True, False):
                act(block_msg(up, blk, h, False, t))

    BP = [(cx, dy) for dy in (2, 1, 3, 0) for cx in (0, 1) if (cx, dy) != (0, 0)]

    def bcols(cx, dy, blk):
        yy = rel(y, dy, Y)
        return b_in.at[:, pl.ds(pl.multiple_of((yy * 2 + core(cx)) * nd + blk * nb, nb), nb)]

    def bpiece(blk, cx, dy):
        m = cx * Y + (Y - dy) % Y
        dst = b_buf.at[blk, m, pl.ds(pl.multiple_of(z * rb, rb), rb), :]
        return remote(bcols(cx, dy, blk), dst, bs, br.at[blk], dev(cx=cx, dy=dy))

    def bown(blk):
        return pltpu.make_async_copy(
            bcols(0, 0, blk), b_buf.at[blk, 0, pl.ds(pl.multiple_of(z * rb, rb), rb), :], bo)

    def bstart(blk):
        for cx, dy in BP:
            bpiece(blk, cx, dy).start()

    def bwait(blk):
        landed(b_buf.at[blk, pl.ds(1, 2 * Y - 1), pl.ds(pl.multiple_of(z * rb, rb), rb), :], br.at[blk])

    def aslot(yr, k, cc):
        dd = 2 * rel(x, -k, X) + cc
        return a_buf.at[rel(y, yr, Y), pl.ds(pl.multiple_of(dd * ra, ra), ra), :]

    def acols(xx):
        return a_in.at[:, pl.ds(pl.multiple_of(xx * kx, kx), kx)]

    def ax(k):
        return remote(acols(rel(x, k, X)), aslot(0, 0, c), as7, axr.at[k], dev(dx=k))

    def asrc(yr, k):
        if yr == 0 and k == 0:
            return acols(x)
        return aslot(yr, k, c)

    def ay(up, k):
        return remote(asrc(0, k), aslot(0, k, c), as24, ayr.at[up, k], dev(dy=1 if up else -1))

    def fy(k):
        up = k in (0, 2)
        ref = aslot(-1 if up else 1, k, c)
        return remote(ref, ref, as7, fyr.at[k], dev(dy=1 if up else -1))

    def ad(yr, k):
        return remote(asrc(yr, k), aslot(yr, k, c), as24, adr.at[yr], dev(cx=1))

    def aown():
        return pltpu.make_async_copy(acols(x), aslot(0, 0, c), axr.at[0])

    class Tiles:
        def __init__(self, c_, rp, rm, fp, fm, s_, rss, rsr, rsf, oss, osr, first, width):
            self.c, self.rp, self.rm, self.fp, self.fm, self.s = c_, rp, rm, fp, fm, s_
            self.rss, self.rsr, self.rsf, self.oss, self.osr = rss, rsr, rsf, oss, osr
            self.first, self.width = first, width

        def rows(self, q, dx, cc):
            dd = 2 * rel(x, dx, X) + cc
            return self.c.at[q, pl.ds(pl.multiple_of(dd * ra, ra), ra), :]

        def part(self, q, m):
            src = (self.rows(q, 2, 0), self.rows(q, 2, 1), self.rows(q, 1, 1),
                   self.rows(q, -1, 0), self.rows(q, 1, 0), self.rows(q, -1, 1))[m]
            dst = (self.rp.at[q], self.rm.at[q], self.fp.at[q, 1],
                   self.fm.at[q, 0], self.fp.at[q, 0], self.fm.at[q, 1])[m]
            return remote(src, dst, self.rss, (self.rsr if m < 2 else self.rsf).at[q], dev(dx=1 if m % 2 == 0 else -1))

        def place(self, q):
            n = nb * self.width
            col = (2 * y + c) * nd + (self.first + (q // Y) * self.width) * nb
            return out.at[:, pl.ds(pl.multiple_of(col, nb), n)]

        def piece(self, q, cx):
            return remote(self.s.at[q, cx], self.place(q), self.oss, self.osr, dev(cx=cx, dy=lax.rem(q, Y)))

        def tile(self, q):
            blk = self.first + (q // Y) * self.width
            yy = rel(y, lax.rem(q, Y), Y)
            total = None
            for m in range(2 * Y):
                src = core(m // Y) * Y + rel(y, m % Y, Y)
                lhs = a_buf[yy, :, pl.ds(pl.multiple_of(src * kb, kb), kb)]
                rhs = [b_buf[blk + i, m] for i in range(self.width)]
                rhs = rhs[0] if self.width == 1 else jnp.concatenate(rhs, axis=1)
                part = jnp.dot(lhs, rhs, preferred_element_type=jnp.float32)
                total = part if total is None else total + part
            self.c[q] = total

        def send(self, q):
            for m in range(4):
                self.part(q, m).start()

        def relay(self, q):
            landed(self.c.at[q, pl.ds(0, 2 * ra), :], self.rsr.at[q])
            u, v = self.rows(q, 1, 0), self.rows(q, -1, 1)
            u[...] = u[...] + self.rp[q]
            v[...] = v[...] + self.rm[q]

        def send_relayed(self, q):
            self.part(q, 4).start()
            self.part(q, 5).start()

        def finish(self, q):
            landed(self.c.at[q, pl.ds(0, 4 * ra), :], self.rsf.at[q])
            for cx in range(2):
                cc = core(cx)
                total = self.rows(q, 0, cc)[...] + self.fp[q, cc] + self.fm[q, cc]
                self.s[q, cx] = total.astype(self.s.dtype)

        def output(self, q):
            self.piece(q, 1).start()

            @pl.when(lax.rem(q, Y) == 0)
            def _():
                self.place(q)[...] = self.s[q, 0]

            @pl.when(lax.rem(q, Y) != 0)
            def _():
                self.piece(q, 0).start()

        def end(self, tiles):
            left(self.c.at[pl.ds(0, tiles * 6 // (2 * X)), :, :], self.rss)
            left(self.s.at[pl.ds(0, tiles * 7 // 8)], self.oss)
            landed(self.s.at[pl.ds(0, tiles * 7 // 8)], self.osr)

    two = Tiles(c2, rp2, rm2, fp2, fm2, s2_, rss2, rsr2, rsf2, oss2, osr2, 0, 2)
    one = Tiles(c1, rp1, rm1, fp1, fm1, s1_, rss1, rsr1, rsf1, oss1, osr1, 2 * PAIRS, 1)

    peers = [dict(dx=1), dict(dx=2), dict(dx=3), dict(dz=1), dict(dz=-1)]
    peers += [dict(cx=cx, dy=dy) for cx, dy in BP]
    barrier = pltpu.get_barrier_semaphore()
    for p in peers:
        pl.semaphore_signal(barrier, inc=1, device_id=dev(**p), device_id_type=pl.DeviceIdType.MESH)
    for blk in range(BLOCKS):
        bown(blk).start()
    aown().start()
    landed(b_buf.at[:, 0, pl.ds(pl.multiple_of(z * rb, rb), rb), :], bo)
    pl.semaphore_wait(barrier, len(peers))

    def a_first():
        ax(1).start()
        ax(3).start()
        for blk in range(3):
            bstart(blk)
        ay(1, 0).start()
        ay(0, 0).start()
        ad(0, 0).start()

    def a_far():
        ax(2).start()

    def a_x(k):
        ax(k).wait_recv()
        ay(1, k).start()
        ay(0, k).start()
        ad(0, k).start()

    def a_y(k):
        ay(1, k).wait_recv()
        ay(0, k).wait_recv()
        fy(k).start()
        ad(3, k).start()
        ad(1, k).start()

    def a_f(k):
        fy(k).wait_recv()
        ad(2, k).start()

    def a_rows(yr):
        if yr == 0:
            aown().wait()
        landed(a_buf.at[0, pl.ds(0, X * ra), :], adr.at[yr])

    def start(m):
        m.start()

    def recv(m):
        m.wait_recv()

    def sent(m):
        m.wait_send()

    def last_hop(h, i, act):
        for up in (True, False):
            act(last_msg(up, h, i))

    def run(t, group):
        for at, calls in group.items():
            @pl.when(t == at)
            def _():
                for fn, *arg in calls:
                    fn(*arg)

    ahead = {0: [(a_first,)], 3: [(a_far,)], 6: [(a_x, 1), (a_x, 3)], 12: [(a_x, 2)], 13: [(a_y, 0), (a_y, 1)], 16: [(a_y, 3)],
             20: [(a_y, 2)]}
    beside = {FIRST: [(a_rows, 0), (a_rows, 1), (a_rows, 3)], 27: [(a_f, 0), (a_f, 1)], 30: [(a_f, 3), (a_f, 2)],
              FIRST + 10: [(a_rows, 2)]}
    tail = {42: [(last_hop, 1, 0, recv), (last_hop, 2, 0, start)],
            45: [(last_hop, 1, 1, recv), (last_hop, 2, 1, start)],
            46: [(last_hop, 2, 0, recv), (last_hop, 1, 0, sent), (last_hop, 3, 0, start)],
            48: [(last_hop, 2, 1, recv), (last_hop, 1, 1, sent)], 50: [(last_hop, 3, 0, recv)]}
    last_slot = SINGLE + 6 * (BLOCKS - 2 * PAIRS - 1) + Y - 1

    def pair_stage(slot, name, lag):
        w = slot - lag
        i, r = w // 4, lax.rem(w, 4)
        late, last = i // 5, i // 7
        q = (1 - late) * (Y * (i - 2 * (i // 4)) + r + r // 2) + (late - last) * (Y * r + 2) + last * (12 + r)
        some = (r < 3) & ((i < 2) | (i == 4) | (i == 5))

        @pl.when((w >= 0) & (w < 32) & (some | (i == 7)))
        def _():
            getattr(two, name)(q)

    def block_stage(slot, name, lag, first=0, last=BLOCKS - 2 * PAIRS):
        v = slot - SINGLE - lag
        k, r = v // 6, lax.rem(v, 6)

        @pl.when((v >= 6 * first) & (k < last) & (r < Y))
        def _():
            getattr(one, name)(Y * k + r)

    def both_stages(slot, name, lag, last_lag):
        n = BLOCKS - 2 * PAIRS
        block_stage(slot, name, lag, 0, n - 1)
        block_stage(slot, name, last_lag, n - 1, n)

    def slots(slot, carry):
        @pl.when(slot < 32 + 12)
        def _():
            pair_stage(slot, "send", 1)
            pair_stage(slot, "send_relayed", 7)
            pair_stage(slot, "output", 12)
            pair_stage(slot, "relay", 6)
            pair_stage(slot, "finish", 11)
            pair_stage(slot, "tile", 0)

        @pl.when(slot >= SINGLE)
        def _():
            block_stage(slot, "send", 1)

            @pl.when((slot >= 42) & (slot <= 50))
            def _():
                run(slot, tail)

            both_stages(slot, "send_relayed", 6, 5)
            both_stages(slot, "output", 12, 9)
            block_stage(slot, "tile", 0)
            both_stages(slot, "relay", 5, 4)
            both_stages(slot, "finish", 11, 8)

        return carry

    def tick(t, carry):
        @pl.when(t < END + 2)
        def _():
            ring(t - 2, recv)
            ring(t - 4, sent)
            ahead3 = lax.rem(t, 3)

            @pl.when((ahead3 == 0) & (t >= LEAD) & (t < LEAD + 3 * BLOCKS))
            def _():
                bwait((t - LEAD) // 3)

            @pl.when(t < END)
            def _():
                ring(t, start)

            @pl.when(t == END - 2)
            def _():
                last_hop(1, 0, start)

            @pl.when(t == END - 1)
            def _():
                last_hop(1, 1, start)

            @pl.when((ahead3 == 1) & (t < 3 * (BLOCKS - 3)))
            def _():
                bstart((t + 8) // 3)

            @pl.when(t < FIRST)
            def _():
                run(t, ahead)

            @pl.when(t >= FIRST)
            def _():
                run(t, beside)

        @pl.when(t >= FIRST)
        def _():
            first = 2 * (t - FIRST)
            lax.fori_loop(first, first + 2, slots, None)

        return carry

    lax.fori_loop(0, FIRST + (last_slot + 9) // 2 + 1, tick, None)

    def ring_sent(t, carry):
        ring(t, sent)
        return carry

    lax.fori_loop(END - 1, END, ring_sent, None)
    for h, i in ((2, 0), (2, 1), (3, 0)):
        last_hop(h, i, sent)
    left(b_buf.at[:, pl.ds(1, 2 * Y - 1), pl.ds(0, rb), :], bs)
    left(a_buf.at[pl.ds(0, 3)], as24)
    left(a_buf.at[0, pl.ds(0, 7 * ra), :], as7)
    two.end(PT)
    one.end(ST)


def solution(mesh):
    all_axes = ("depth", "row", "col")

    def device_block(a_rows, b_rows):
        ra, k = a_rows.shape
        rb, n = b_rows.shape
        nb = n // (2 * Y) // BLOCKS
        dma = pltpu.SemaphoreType.DMA
        f32, bf16 = jnp.float32, a_rows.dtype

        def both(*tail, dtype):
            return [pltpu.VMEM((PT, *tail, 2 * nb), dtype), pltpu.VMEM((ST, *tail, nb), dtype)]

        scratch = [
            pltpu.VMEM((Y, 2 * X * ra, k // X), bf16),
            pltpu.VMEM((BLOCKS, 2 * Y, Z * rb, nb), bf16),
            *both(2 * X * ra, dtype=f32),
            *both(ra, dtype=f32), *both(ra, dtype=f32),
            *both(2, ra, dtype=f32), *both(2, ra, dtype=f32),
            *both(2, ra, dtype=bf16),
            dma((2, 4)), dma((2, 4)), dma((2, 4)), dma((2, 4)),
            dma, dma((BLOCKS,)), dma, dma((X,)), dma((2, X)), dma((X,)), dma((Y,)), dma, dma,
            dma, dma((PT,)), dma((PT,)), dma, dma,
            dma, dma((ST,)), dma((ST,)), dma, dma,
        ]
        return pl.pallas_call(
            kernel,
            out_shape=pltpu.VMEM((ra, n), bf16),
            in_specs=[pl.BlockSpec(memory_space=pl.ANY)] * 2,
            out_specs=pl.BlockSpec(memory_space=pltpu.VMEM),
            scratch_shapes=scratch,
            compiler_params=pltpu.CompilerParams(
                collective_id=0, has_side_effects=True, vmem_limit_bytes=62000000),
        )(a_rows, b_rows)

    return jax.shard_map(device_block, mesh=mesh, in_specs=(P(all_axes, None), P(all_axes, None)),
                         out_specs=P(all_axes, None), check_vma=False)
```

```python
import jax
import jax.numpy as jnp
from jax import lax
from jax.experimental import pallas as pl
from jax.experimental.pallas import tpu as pltpu
from jax.sharding import PartitionSpec as P

X = 4
Y = 4
Z = 8
BLOCKS = 12
PAIRS = 4
LEAD = 6
END = 43
FIRST = 22
SINGLE = 32
PT = PAIRS * Y
ST = (BLOCKS - 2 * PAIRS) * Y


def kernel(a_in, b_in, out, a_buf, b_buf, c2, c1, rp2, rp1, rm2, rm1, fp2, fp1, fm2, fm1, s2_, s1_,
           zps, zpr, zms, zmr, bs, br, bo, axr, ayr, fyr, adr, as24, as7,
           rss2, rsr2, rsf2, oss2, osr2, rss1, rsr1, rsf1, oss1, osr1):
    d = lax.axis_index("depth")
    y = lax.axis_index("row")
    z = lax.axis_index("col")
    x = d // 2
    c = lax.rem(d, 2)
    ra = a_in.shape[0]
    rb = b_in.shape[0]
    kx = a_in.shape[1] // X
    nd = b_in.shape[1] // (2 * Y)
    nb = nd // BLOCKS
    kb = Z * rb

    def rel(v, k, n):
        return lax.rem(v + k + n, n)

    def core(cx):
        return c if cx == 0 else 1 - c

    def dev(dx=0, cx=0, dy=0, dz=0):
        xx = x if isinstance(dx, int) and dx == 0 else rel(x, dx, X)
        yy = y if isinstance(dy, int) and dy == 0 else rel(y, dy, Y)
        zz = z if isinstance(dz, int) and dz == 0 else rel(z, dz, Z)
        return {"depth": 2 * xx + core(cx), "row": yy, "col": zz}

    def remote(src, dst, ss, rs, device):
        return pltpu.make_async_remote_copy(
            src_ref=src, dst_ref=dst, send_sem=ss, recv_sem=rs,
            device_id=device, device_id_type=pl.DeviceIdType.MESH)

    def landed(ref, sem):
        remote(ref, ref, bs, sem, dev(dz=1)).wait_recv()

    def left(ref, sem):
        remote(ref, ref, sem, bo, dev(dz=1)).wait_send()

    def sems(up, kind, t):
        ss, rs = (zps, zpr) if up else (zms, zmr)
        return ss.at[kind, lax.rem(t, 4)], rs.at[kind, lax.rem(t, 4)]

    def own_msg(up, i, t):
        s = lax.rem(i, 2) if up else 1 - lax.rem(i, 2)
        sh = rel(z, -(i // 2) if up else i // 2, Z)
        half = BLOCKS // 2
        ref = b_buf.at[pl.ds(half * s, half), 0, pl.ds(pl.multiple_of(sh * rb, rb), rb), :]
        return remote(ref, ref, *sems(up, 0, t), dev(dz=1 if up else -1))

    def block_msg(up, blk, h, half, t):
        sh = rel(z, -h if up else h, Z)
        if half:
            n = rb // 2
            off = sh * rb + (0 if up else n)
        else:
            n, off = rb, sh * rb
        ref = b_buf.at[blk, pl.ds(1, 2 * Y - 1), pl.ds(pl.multiple_of(off, n), n), :]
        return remote(ref, ref, *sems(up, 1 if half else 0, t), dev(dz=1 if up else -1))

    def last_msg(up, h, i):
        sh = rel(z, -h if up else h, Z)
        n = rb // 2
        off = sh * rb + n * (i if up else 1 - i)
        ref = b_buf.at[BLOCKS - 1, pl.ds(1, 2 * Y - 1), pl.ds(pl.multiple_of(off, n), n), :]
        return remote(ref, ref, *sems(up, i, END - 4 + 2 * h), dev(dz=1 if up else -1))

    def ring(t, act):
        u = t - LEAD
        odd = lax.rem(u, 2)
        k = (u + 3 * odd) // 2
        blk, h = 2 * (k // 3) - odd, lax.rem(k, 3)
        block = (t >= LEAD) & (blk >= 0)

        @pl.when((t >= 0) & ((t < LEAD) | (blk < 0)))
        def _():
            for up in (True, False):
                act(own_msg(up, t - t // (LEAD + 1), t))

        @pl.when(block & (h == 0) & (blk >= 2))
        def _():
            for up in (True, False):
                act(block_msg(up, blk - 2, 3, True, t))

        @pl.when(block & (3 * blk + h <= 3 * (BLOCKS - 1)))
        def _():
            for up in (True, False):
                act(block_msg(up, blk, h, False, t))

    BP = [(cx, dy) for dy in (2, 1, 3, 0) for cx in (0, 1) if (cx, dy) != (0, 0)]

    def bcols(cx, dy, blk):
        yy = rel(y, dy, Y)
        return b_in.at[:, pl.ds(pl.multiple_of((yy * 2 + core(cx)) * nd + blk * nb, nb), nb)]

    def bpiece(blk, cx, dy):
        m = cx * Y + (Y - dy) % Y
        dst = b_buf.at[blk, m, pl.ds(pl.multiple_of(z * rb, rb), rb), :]
        return remote(bcols(cx, dy, blk), dst, bs, br.at[blk], dev(cx=cx, dy=dy))

    def bown(blk):
        return pltpu.make_async_copy(
            bcols(0, 0, blk), b_buf.at[blk, 0, pl.ds(pl.multiple_of(z * rb, rb), rb), :], bo)

    def bstart(blk):
        for cx, dy in BP:
            bpiece(blk, cx, dy).start()

    def bwait(blk):
        landed(b_buf.at[blk, pl.ds(1, 2 * Y - 1), pl.ds(pl.multiple_of(z * rb, rb), rb), :], br.at[blk])

    def aslot(yr, k, cc):
        dd = 2 * rel(x, -k, X) + cc
        return a_buf.at[rel(y, yr, Y), pl.ds(pl.multiple_of(dd * ra, ra), ra), :]

    def acols(xx):
        return a_in.at[:, pl.ds(pl.multiple_of(xx * kx, kx), kx)]

    def ax(k):
        return remote(acols(rel(x, k, X)), aslot(0, 0, c), as7, axr.at[k], dev(dx=k))

    def asrc(yr, k):
        if yr == 0 and k == 0:
            return acols(x)
        return aslot(yr, k, c)

    def ay(up, k):
        return remote(asrc(0, k), aslot(0, k, c), as24, ayr.at[up, k], dev(dy=1 if up else -1))

    def fy(k):
        up = k in (0, 2)
        ref = aslot(-1 if up else 1, k, c)
        return remote(ref, ref, as7, fyr.at[k], dev(dy=1 if up else -1))

    def ad(yr, k):
        return remote(asrc(yr, k), aslot(yr, k, c), as24, adr.at[yr], dev(cx=1))

    def aown():
        return pltpu.make_async_copy(acols(x), aslot(0, 0, c), axr.at[0])

    class Tiles:
        def __init__(self, c_, rp, rm, fp, fm, s_, rss, rsr, rsf, oss, osr, first, width):
            self.c, self.rp, self.rm, self.fp, self.fm, self.s = c_, rp, rm, fp, fm, s_
            self.rss, self.rsr, self.rsf, self.oss, self.osr = rss, rsr, rsf, oss, osr
            self.first, self.width = first, width

        def rows(self, q, dx, cc):
            dd = 2 * rel(x, dx, X) + cc
            return self.c.at[q, pl.ds(pl.multiple_of(dd * ra, ra), ra), :]

        def part(self, q, m):
            src = (self.rows(q, 2, 0), self.rows(q, 2, 1), self.rows(q, 1, 1),
                   self.rows(q, -1, 0), self.rows(q, 1, 0), self.rows(q, -1, 1))[m]
            dst = (self.rp.at[q], self.rm.at[q], self.fp.at[q, 1],
                   self.fm.at[q, 0], self.fp.at[q, 0], self.fm.at[q, 1])[m]
            return remote(src, dst, self.rss, (self.rsr if m < 2 else self.rsf).at[q], dev(dx=1 if m % 2 == 0 else -1))

        def place(self, q):
            n = nb * self.width
            col = (2 * y + c) * nd + (self.first + (q // Y) * self.width) * nb
            return out.at[:, pl.ds(pl.multiple_of(col, nb), n)]

        def piece(self, q, cx):
            return remote(self.s.at[q, cx], self.place(q), self.oss, self.osr, dev(cx=cx, dy=lax.rem(q, Y)))

        def tile(self, q):
            blk = self.first + (q // Y) * self.width
            yy = rel(y, lax.rem(q, Y), Y)
            total = None
            for m in range(2 * Y):
                src = core(m // Y) * Y + rel(y, m % Y, Y)
                lhs = a_buf[yy, :, pl.ds(pl.multiple_of(src * kb, kb), kb)]
                rhs = [b_buf[blk + i, m] for i in range(self.width)]
                rhs = rhs[0] if self.width == 1 else jnp.concatenate(rhs, axis=1)
                part = jnp.dot(lhs, rhs, preferred_element_type=jnp.float32)
                total = part if total is None else total + part
            self.c[q] = total

        def send(self, q):
            for m in range(4):
                self.part(q, m).start()

        def relay(self, q):
            landed(self.c.at[q, pl.ds(0, 2 * ra), :], self.rsr.at[q])
            u, v = self.rows(q, 1, 0), self.rows(q, -1, 1)
            u[...] = u[...] + self.rp[q]
            v[...] = v[...] + self.rm[q]

        def send_relayed(self, q):
            self.part(q, 4).start()
            self.part(q, 5).start()

        def finish(self, q):
            landed(self.c.at[q, pl.ds(0, 4 * ra), :], self.rsf.at[q])
            for cx in range(2):
                cc = core(cx)
                total = self.rows(q, 0, cc)[...] + self.fp[q, cc] + self.fm[q, cc]
                self.s[q, cx] = total.astype(self.s.dtype)

        def output(self, q):
            self.piece(q, 1).start()

            @pl.when(lax.rem(q, Y) == 0)
            def _():
                self.place(q)[...] = self.s[q, 0]

            @pl.when(lax.rem(q, Y) != 0)
            def _():
                self.piece(q, 0).start()

        def end(self, tiles):
            left(self.c.at[pl.ds(0, tiles * 6 // (2 * X)), :, :], self.rss)
            left(self.s.at[pl.ds(0, tiles * 7 // 8)], self.oss)
            landed(self.s.at[pl.ds(0, tiles * 7 // 8)], self.osr)

    two = Tiles(c2, rp2, rm2, fp2, fm2, s2_, rss2, rsr2, rsf2, oss2, osr2, 0, 2)
    one = Tiles(c1, rp1, rm1, fp1, fm1, s1_, rss1, rsr1, rsf1, oss1, osr1, 2 * PAIRS, 1)

    peers = [dict(dx=1), dict(dx=2), dict(dx=3), dict(dz=1), dict(dz=-1)]
    peers += [dict(cx=cx, dy=dy) for cx, dy in BP]
    barrier = pltpu.get_barrier_semaphore()
    for p in peers:
        pl.semaphore_signal(barrier, inc=1, device_id=dev(**p), device_id_type=pl.DeviceIdType.MESH)
    for blk in range(BLOCKS):
        bown(blk).start()
    aown().start()
    landed(b_buf.at[:, 0, pl.ds(pl.multiple_of(z * rb, rb), rb), :], bo)
    pl.semaphore_wait(barrier, len(peers))

    def a_first():
        ax(1).start()
        ax(3).start()
        for blk in range(3):
            bstart(blk)
        ay(1, 0).start()
        ay(0, 0).start()
        ad(0, 0).start()

    def a_far():
        ax(2).start()

    def a_x(k):
        ax(k).wait_recv()
        ay(1, k).start()
        ay(0, k).start()
        ad(0, k).start()

    def a_y(k):
        ay(1, k).wait_recv()
        ay(0, k).wait_recv()
        fy(k).start()
        ad(3, k).start()
        ad(1, k).start()

    def a_f(k):
        fy(k).wait_recv()
        ad(2, k).start()

    def a_rows(yr):
        if yr == 0:
            aown().wait()
        landed(a_buf.at[0, pl.ds(0, X * ra), :], adr.at[yr])

    def start(m):
        m.start()

    def recv(m):
        m.wait_recv()

    def sent(m):
        m.wait_send()

    def last_hop(h, i, act):
        for up in (True, False):
            act(last_msg(up, h, i))

    def run(t, group):
        for at, calls in group.items():
            @pl.when(t == at)
            def _():
                for fn, *arg in calls:
                    fn(*arg)

    ahead = {0: [(a_first,)], 3: [(a_far,)], 7: [(a_x, 3)], 8: [(a_x, 1)], 12: [(a_x, 2)], 13: [(a_y, 0)], 14: [(a_y, 3)], 17: [(a_y, 1)],
             20: [(a_y, 2)]}
    beside = {FIRST: [(a_rows, 0), (a_rows, 1), (a_rows, 3)], 27: [(a_f, 0), (a_f, 1)], 30: [(a_f, 3), (a_f, 2)],
              FIRST + 10: [(a_rows, 2)]}
    tail = {42: [(last_hop, 1, 0, recv), (last_hop, 2, 0, start)],
            45: [(last_hop, 1, 1, recv), (last_hop, 2, 1, start)],
            46: [(last_hop, 2, 0, recv), (last_hop, 1, 0, sent), (last_hop, 3, 0, start)],
            48: [(last_hop, 2, 1, recv), (last_hop, 1, 1, sent)], 50: [(last_hop, 3, 0, recv)]}
    last_slot = SINGLE + 6 * (BLOCKS - 2 * PAIRS - 1) + Y - 1

    def pair_stage(slot, name, lag):
        w = slot - lag
        i, r = w // 4, lax.rem(w, 4)
        late, last = i // 5, i // 7
        q = (1 - late) * (Y * (i - 2 * (i // 4)) + r + r // 2) + (late - last) * (Y * r + 2) + last * (12 + r)
        some = (r < 3) & ((i < 2) | (i == 4) | (i == 5))

        @pl.when((w >= 0) & (w < 32) & (some | (i == 7)))
        def _():
            getattr(two, name)(q)

    def block_stage(slot, name, lag, first=0, last=BLOCKS - 2 * PAIRS):
        v = slot - SINGLE - lag
        k, r = v // 6, lax.rem(v, 6)

        @pl.when((v >= 6 * first) & (k < last) & (r < Y))
        def _():
            getattr(one, name)(Y * k + r)

    def both_stages(slot, name, lag, last_lag):
        n = BLOCKS - 2 * PAIRS
        block_stage(slot, name, lag, 0, n - 1)
        block_stage(slot, name, last_lag, n - 1, n)

    def slots(slot, carry):
        @pl.when(slot < 32 + 12)
        def _():
            pair_stage(slot, "send", 1)
            pair_stage(slot, "send_relayed", 7)
            pair_stage(slot, "output", 12)
            pair_stage(slot, "relay", 6)
            pair_stage(slot, "finish", 11)
            pair_stage(slot, "tile", 0)

        @pl.when(slot >= SINGLE)
        def _():
            block_stage(slot, "send", 1)

            @pl.when((slot >= 42) & (slot <= 50))
            def _():
                run(slot, tail)

            both_stages(slot, "send_relayed", 6, 5)
            both_stages(slot, "output", 12, 9)
            block_stage(slot, "tile", 0)
            both_stages(slot, "relay", 5, 4)
            both_stages(slot, "finish", 11, 8)

        return carry

    def tick(t, carry):
        @pl.when(t < END + 2)
        def _():
            ring(t - 2, recv)
            ring(t - 4, sent)
            ahead3 = lax.rem(t, 3)

            @pl.when((ahead3 == 0) & (t >= LEAD) & (t < LEAD + 3 * BLOCKS))
            def _():
                bwait((t - LEAD) // 3)

            @pl.when(t < END)
            def _():
                ring(t, start)

            @pl.when(t == END - 2)
            def _():
                last_hop(1, 0, start)

            @pl.when(t == END - 1)
            def _():
                last_hop(1, 1, start)

            @pl.when((ahead3 == 1) & (t < 3 * (BLOCKS - 3)))
            def _():
                bstart((t + 8) // 3)

            @pl.when(t < FIRST)
            def _():
                run(t, ahead)

            @pl.when(t >= FIRST)
            def _():
                run(t, beside)

        @pl.when(t >= FIRST)
        def _():
            first = 2 * (t - FIRST)
            lax.fori_loop(first, first + 2, slots, None)

        return carry

    lax.fori_loop(0, FIRST + (last_slot + 9) // 2 + 1, tick, None)

    def ring_sent(t, carry):
        ring(t, sent)
        return carry

    lax.fori_loop(END - 1, END, ring_sent, None)
    for h, i in ((2, 0), (2, 1), (3, 0)):
        last_hop(h, i, sent)
    left(b_buf.at[:, pl.ds(1, 2 * Y - 1), pl.ds(0, rb), :], bs)
    left(a_buf.at[pl.ds(0, 3)], as24)
    left(a_buf.at[0, pl.ds(0, 7 * ra), :], as7)
    two.end(PT)
    one.end(ST)


def solution(mesh):
    all_axes = ("depth", "row", "col")

    def device_block(a_rows, b_rows):
        ra, k = a_rows.shape
        rb, n = b_rows.shape
        nb = n // (2 * Y) // BLOCKS
        dma = pltpu.SemaphoreType.DMA
        f32, bf16 = jnp.float32, a_rows.dtype

        def both(*tail, dtype):
            return [pltpu.VMEM((PT, *tail, 2 * nb), dtype), pltpu.VMEM((ST, *tail, nb), dtype)]

        scratch = [
            pltpu.VMEM((Y, 2 * X * ra, k // X), bf16),
            pltpu.VMEM((BLOCKS, 2 * Y, Z * rb, nb), bf16),
            *both(2 * X * ra, dtype=f32),
            *both(ra, dtype=f32), *both(ra, dtype=f32),
            *both(2, ra, dtype=f32), *both(2, ra, dtype=f32),
            *both(2, ra, dtype=bf16),
            dma((2, 4)), dma((2, 4)), dma((2, 4)), dma((2, 4)),
            dma, dma((BLOCKS,)), dma, dma((X,)), dma((2, X)), dma((X,)), dma((Y,)), dma, dma,
            dma, dma((PT,)), dma((PT,)), dma, dma,
            dma, dma((ST,)), dma((ST,)), dma, dma,
        ]
        return pl.pallas_call(
            kernel,
            out_shape=pltpu.VMEM((ra, n), bf16),
            in_specs=[pl.BlockSpec(memory_space=pl.ANY)] * 2,
            out_specs=pl.BlockSpec(memory_space=pltpu.VMEM),
            scratch_shapes=scratch,
            compiler_params=pltpu.CompilerParams(
                collective_id=0, has_side_effects=True, vmem_limit_bytes=62000000),
        )(a_rows, b_rows)

    return jax.shard_map(device_block, mesh=mesh, in_specs=(P(all_axes, None), P(all_axes, None)),
                         out_specs=P(all_axes, None), check_vma=False)
```

```python
import jax
import jax.numpy as jnp
from jax import lax
from jax.experimental import pallas as pl
from jax.experimental.pallas import tpu as pltpu
from jax.sharding import PartitionSpec as P

X = 4
Y = 4
Z = 8
BLOCKS = 12
PAIRS = 4
LEAD = 6
END = 43
FIRST = 22
SINGLE = 32
PT = PAIRS * Y
ST = (BLOCKS - 2 * PAIRS) * Y


def kernel(a_in, b_in, out, a_buf, b_buf, c2, c1, rp2, rp1, rm2, rm1, fp2, fp1, fm2, fm1, s2_, s1_,
           zps, zpr, zms, zmr, bs, br, bo, axr, ayr, fyr, adr, as24, as7,
           rss2, rsr2, rsf2, oss2, osr2, rss1, rsr1, rsf1, oss1, osr1):
    d = lax.axis_index("depth")
    y = lax.axis_index("row")
    z = lax.axis_index("col")
    x = d // 2
    c = lax.rem(d, 2)
    ra = a_in.shape[0]
    rb = b_in.shape[0]
    kx = a_in.shape[1] // X
    nd = b_in.shape[1] // (2 * Y)
    nb = nd // BLOCKS
    kb = Z * rb

    def rel(v, k, n):
        return lax.rem(v + k + n, n)

    def core(cx):
        return c if cx == 0 else 1 - c

    def dev(dx=0, cx=0, dy=0, dz=0):
        xx = x if isinstance(dx, int) and dx == 0 else rel(x, dx, X)
        yy = y if isinstance(dy, int) and dy == 0 else rel(y, dy, Y)
        zz = z if isinstance(dz, int) and dz == 0 else rel(z, dz, Z)
        return {"depth": 2 * xx + core(cx), "row": yy, "col": zz}

    def remote(src, dst, ss, rs, device):
        return pltpu.make_async_remote_copy(
            src_ref=src, dst_ref=dst, send_sem=ss, recv_sem=rs,
            device_id=device, device_id_type=pl.DeviceIdType.MESH)

    def landed(ref, sem):
        remote(ref, ref, bs, sem, dev(dz=1)).wait_recv()

    def left(ref, sem):
        remote(ref, ref, sem, bo, dev(dz=1)).wait_send()

    def sems(up, kind, t):
        ss, rs = (zps, zpr) if up else (zms, zmr)
        return ss.at[kind, lax.rem(t, 4)], rs.at[kind, lax.rem(t, 4)]

    def own_msg(up, i, t):
        s = lax.rem(i, 2) if up else 1 - lax.rem(i, 2)
        sh = rel(z, -(i // 2) if up else i // 2, Z)
        half = BLOCKS // 2
        ref = b_buf.at[pl.ds(half * s, half), 0, pl.ds(pl.multiple_of(sh * rb, rb), rb), :]
        return remote(ref, ref, *sems(up, 0, t), dev(dz=1 if up else -1))

    def block_msg(up, blk, h, half, t):
        sh = rel(z, -h if up else h, Z)
        if half:
            n = rb // 2
            off = sh * rb + (0 if up else n)
        else:
            n, off = rb, sh * rb
        ref = b_buf.at[blk, pl.ds(1, 2 * Y - 1), pl.ds(pl.multiple_of(off, n), n), :]
        return remote(ref, ref, *sems(up, 1 if half else 0, t), dev(dz=1 if up else -1))

    def last_msg(up, h, i):
        sh = rel(z, -h if up else h, Z)
        n = rb // 2
        off = sh * rb + n * (i if up else 1 - i)
        ref = b_buf.at[BLOCKS - 1, pl.ds(1, 2 * Y - 1), pl.ds(pl.multiple_of(off, n), n), :]
        return remote(ref, ref, *sems(up, i, END - 4 + 2 * h), dev(dz=1 if up else -1))

    def ring(t, act):
        u = t - LEAD
        odd = lax.rem(u, 2)
        k = (u + 3 * odd) // 2
        blk, h = 2 * (k // 3) - odd, lax.rem(k, 3)
        block = (t >= LEAD) & (blk >= 0)

        @pl.when((t >= 0) & ((t < LEAD) | (blk < 0)))
        def _():
            for up in (True, False):
                act(own_msg(up, t - t // (LEAD + 1), t))

        @pl.when(block & (h == 0) & (blk >= 2))
        def _():
            for up in (True, False):
                act(block_msg(up, blk - 2, 3, True, t))

        @pl.when(block & (3 * blk + h <= 3 * (BLOCKS - 1)))
        def _():
            for up in (True, False):
                act(block_msg(up, blk, h, False, t))

    BP = [(cx, dy) for dy in (2, 1, 3, 0) for cx in (0, 1) if (cx, dy) != (0, 0)]

    def bcols(cx, dy, blk):
        yy = rel(y, dy, Y)
        return b_in.at[:, pl.ds(pl.multiple_of((yy * 2 + core(cx)) * nd + blk * nb, nb), nb)]

    def bpiece(blk, cx, dy):
        m = cx * Y + (Y - dy) % Y
        dst = b_buf.at[blk, m, pl.ds(pl.multiple_of(z * rb, rb), rb), :]
        return remote(bcols(cx, dy, blk), dst, bs, br.at[blk], dev(cx=cx, dy=dy))

    def bown(blk):
        return pltpu.make_async_copy(
            bcols(0, 0, blk), b_buf.at[blk, 0, pl.ds(pl.multiple_of(z * rb, rb), rb), :], bo)

    def bstart(blk):
        for cx, dy in BP:
            bpiece(blk, cx, dy).start()

    def bwait(blk):
        landed(b_buf.at[blk, pl.ds(1, 2 * Y - 1), pl.ds(pl.multiple_of(z * rb, rb), rb), :], br.at[blk])

    def aslot(yr, k, cc):
        dd = 2 * rel(x, -k, X) + cc
        return a_buf.at[rel(y, yr, Y), pl.ds(pl.multiple_of(dd * ra, ra), ra), :]

    def acols(xx):
        return a_in.at[:, pl.ds(pl.multiple_of(xx * kx, kx), kx)]

    def ax(k):
        return remote(acols(rel(x, k, X)), aslot(0, 0, c), as7, axr.at[k], dev(dx=k))

    def asrc(yr, k):
        if yr == 0 and k == 0:
            return acols(x)
        return aslot(yr, k, c)

    def ay(up, k):
        return remote(asrc(0, k), aslot(0, k, c), as24, ayr.at[up, k], dev(dy=1 if up else -1))

    def fy(k):
        up = k in (0, 2)
        ref = aslot(-1 if up else 1, k, c)
        return remote(ref, ref, as7, fyr.at[k], dev(dy=1 if up else -1))

    def ad(yr, k):
        return remote(asrc(yr, k), aslot(yr, k, c), as24, adr.at[yr], dev(cx=1))

    def aown():
        return pltpu.make_async_copy(acols(x), aslot(0, 0, c), axr.at[0])

    class Tiles:
        def __init__(self, c_, rp, rm, fp, fm, s_, rss, rsr, rsf, oss, osr, first, width):
            self.c, self.rp, self.rm, self.fp, self.fm, self.s = c_, rp, rm, fp, fm, s_
            self.rss, self.rsr, self.rsf, self.oss, self.osr = rss, rsr, rsf, oss, osr
            self.first, self.width = first, width

        def rows(self, q, dx, cc):
            dd = 2 * rel(x, dx, X) + cc
            return self.c.at[q, pl.ds(pl.multiple_of(dd * ra, ra), ra), :]

        def part(self, q, m):
            src = (self.rows(q, 2, 0), self.rows(q, 2, 1), self.rows(q, 1, 1),
                   self.rows(q, -1, 0), self.rows(q, 1, 0), self.rows(q, -1, 1))[m]
            dst = (self.rp.at[q], self.rm.at[q], self.fp.at[q, 1],
                   self.fm.at[q, 0], self.fp.at[q, 0], self.fm.at[q, 1])[m]
            return remote(src, dst, self.rss, (self.rsr if m < 2 else self.rsf).at[q], dev(dx=1 if m % 2 == 0 else -1))

        def place(self, q):
            n = nb * self.width
            col = (2 * y + c) * nd + (self.first + (q // Y) * self.width) * nb
            return out.at[:, pl.ds(pl.multiple_of(col, nb), n)]

        def piece(self, q, cx):
            return remote(self.s.at[q, cx], self.place(q), self.oss, self.osr, dev(cx=cx, dy=lax.rem(q, Y)))

        def tile(self, q):
            blk = self.first + (q // Y) * self.width
            yy = rel(y, lax.rem(q, Y), Y)
            total = None
            for m in range(2 * Y):
                src = core(m // Y) * Y + rel(y, m % Y, Y)
                lhs = a_buf[yy, :, pl.ds(pl.multiple_of(src * kb, kb), kb)]
                rhs = [b_buf[blk + i, m] for i in range(self.width)]
                rhs = rhs[0] if self.width == 1 else jnp.concatenate(rhs, axis=1)
                part = jnp.dot(lhs, rhs, preferred_element_type=jnp.float32)
                total = part if total is None else total + part
            self.c[q] = total

        def send(self, q):
            for m in range(4):
                self.part(q, m).start()

        def relay(self, q):
            landed(self.c.at[q, pl.ds(0, 2 * ra), :], self.rsr.at[q])
            u, v = self.rows(q, 1, 0), self.rows(q, -1, 1)
            u[...] = u[...] + self.rp[q]
            v[...] = v[...] + self.rm[q]

        def send_relayed(self, q):
            self.part(q, 4).start()
            self.part(q, 5).start()

        def finish(self, q):
            landed(self.c.at[q, pl.ds(0, 4 * ra), :], self.rsf.at[q])
            for cx in range(2):
                cc = core(cx)
                total = self.rows(q, 0, cc)[...] + self.fp[q, cc] + self.fm[q, cc]
                self.s[q, cx] = total.astype(self.s.dtype)

        def output(self, q):
            self.piece(q, 1).start()

            @pl.when(lax.rem(q, Y) == 0)
            def _():
                self.place(q)[...] = self.s[q, 0]

            @pl.when(lax.rem(q, Y) != 0)
            def _():
                self.piece(q, 0).start()

        def end(self, tiles):
            left(self.c.at[pl.ds(0, tiles * 6 // (2 * X)), :, :], self.rss)
            left(self.s.at[pl.ds(0, tiles * 7 // 8)], self.oss)
            landed(self.s.at[pl.ds(0, tiles * 7 // 8)], self.osr)

    two = Tiles(c2, rp2, rm2, fp2, fm2, s2_, rss2, rsr2, rsf2, oss2, osr2, 0, 2)
    one = Tiles(c1, rp1, rm1, fp1, fm1, s1_, rss1, rsr1, rsf1, oss1, osr1, 2 * PAIRS, 1)

    peers = [dict(dx=1), dict(dx=2), dict(dx=3), dict(dz=1), dict(dz=-1)]
    peers += [dict(cx=cx, dy=dy) for cx, dy in BP]
    barrier = pltpu.get_barrier_semaphore()
    for p in peers:
        pl.semaphore_signal(barrier, inc=1, device_id=dev(**p), device_id_type=pl.DeviceIdType.MESH)
    for blk in range(BLOCKS):
        bown(blk).start()
    aown().start()
    landed(b_buf.at[:, 0, pl.ds(pl.multiple_of(z * rb, rb), rb), :], bo)
    pl.semaphore_wait(barrier, len(peers))

    def a_first():
        ax(1).start()
        ax(3).start()
        for blk in range(3):
            bstart(blk)
        ay(1, 0).start()
        ay(0, 0).start()
        ad(0, 0).start()

    def a_far():
        ax(2).start()

    def a_x(k):
        ax(k).wait_recv()
        ay(1, k).start()
        ay(0, k).start()
        ad(0, k).start()

    def a_y(k):
        ay(1, k).wait_recv()
        ay(0, k).wait_recv()
        fy(k).start()
        ad(3, k).start()
        ad(1, k).start()

    def a_f(k):
        fy(k).wait_recv()
        ad(2, k).start()

    def a_rows(yr):
        if yr == 0:
            aown().wait()
        landed(a_buf.at[0, pl.ds(0, X * ra), :], adr.at[yr])

    def start(m):
        m.start()

    def recv(m):
        m.wait_recv()

    def sent(m):
        m.wait_send()

    def last_hop(h, i, act):
        for up in (True, False):
            act(last_msg(up, h, i))

    def run(t, group):
        for at, calls in group.items():
            @pl.when(t == at)
            def _():
                for fn, *arg in calls:
                    fn(*arg)

    ahead = {0: [(a_first,)], 3: [(a_far,)], 7: [(a_x, 3)], 8: [(a_x, 1)], 12: [(a_x, 2)], 13: [(a_y, 0)], 14: [(a_y, 3)], 17: [(a_y, 1)],
             20: [(a_y, 2)]}
    beside = {FIRST: [(a_rows, 0), (a_rows, 1), (a_rows, 3)], 27: [(a_f, 0), (a_f, 1)], 30: [(a_f, 3), (a_f, 2)],
              FIRST + 10: [(a_rows, 2)]}
    tail = {42: [(last_hop, 1, 0, recv), (last_hop, 2, 0, start)],
            45: [(last_hop, 1, 1, recv), (last_hop, 2, 1, start)],
            46: [(last_hop, 2, 0, recv), (last_hop, 1, 0, sent), (last_hop, 3, 0, start)],
            48: [(last_hop, 2, 1, recv), (last_hop, 1, 1, sent)], 50: [(last_hop, 3, 0, recv)]}
    last_slot = SINGLE + 6 * (BLOCKS - 2 * PAIRS - 1) + Y - 1

    def pair_stage(slot, name, lag):
        w = slot - lag
        i, r = w // 4, lax.rem(w, 4)
        late, last = i // 5, i // 7
        q = (1 - late) * (Y * (i - 2 * (i // 4)) + r + r // 2) + (late - last) * (Y * r + 2) + last * (12 + r)
        some = (r < 3) & ((i < 2) | (i == 4) | (i == 5))

        @pl.when((w >= 0) & (w < 32) & (some | (i == 7)))
        def _():
            getattr(two, name)(q)

    def block_stage(slot, name, lag, first=0, last=BLOCKS - 2 * PAIRS):
        v = slot - SINGLE - lag
        k, r = v // 6, lax.rem(v, 6)

        @pl.when((v >= 6 * first) & (k < last) & (r < Y))
        def _():
            getattr(one, name)(Y * k + Y - 1 - r)

    def both_stages(slot, name, lag, last_lag):
        n = BLOCKS - 2 * PAIRS
        block_stage(slot, name, lag, 0, n - 1)
        block_stage(slot, name, last_lag, n - 1, n)

    def slots(slot, carry):
        @pl.when(slot < 32 + 12)
        def _():
            pair_stage(slot, "send", 1)
            pair_stage(slot, "send_relayed", 7)
            pair_stage(slot, "output", 12)
            pair_stage(slot, "relay", 6)
            pair_stage(slot, "finish", 11)
            pair_stage(slot, "tile", 0)

        @pl.when(slot >= SINGLE)
        def _():
            block_stage(slot, "send", 1)

            @pl.when((slot >= 42) & (slot <= 50))
            def _():
                run(slot, tail)

            both_stages(slot, "send_relayed", 5, 5)
            both_stages(slot, "output", 12, 9)
            block_stage(slot, "tile", 0)
            both_stages(slot, "relay", 4, 4)
            both_stages(slot, "finish", 11, 8)

        return carry

    def tick(t, carry):
        @pl.when(t < END + 2)
        def _():
            ring(t - 2, recv)
            ring(t - 4, sent)
            ahead3 = lax.rem(t, 3)

            @pl.when((ahead3 == 0) & (t >= LEAD) & (t < LEAD + 3 * BLOCKS))
            def _():
                bwait((t - LEAD) // 3)

            @pl.when(t < END)
            def _():
                ring(t, start)

            @pl.when(t == END - 2)
            def _():
                last_hop(1, 0, start)

            @pl.when(t == END - 1)
            def _():
                last_hop(1, 1, start)

            @pl.when((ahead3 == 1) & (t < 3 * (BLOCKS - 3)))
            def _():
                bstart((t + 8) // 3)

            @pl.when(t < FIRST)
            def _():
                run(t, ahead)

            @pl.when(t >= FIRST)
            def _():
                run(t, beside)

        @pl.when(t >= FIRST)
        def _():
            first = 2 * (t - FIRST)
            lax.fori_loop(first, first + 2, slots, None)

        return carry

    lax.fori_loop(0, FIRST + (last_slot + 9) // 2 + 1, tick, None)

    def ring_sent(t, carry):
        ring(t, sent)
        return carry

    lax.fori_loop(END - 1, END, ring_sent, None)
    for h, i in ((2, 0), (2, 1), (3, 0)):
        last_hop(h, i, sent)
    left(b_buf.at[:, pl.ds(1, 2 * Y - 1), pl.ds(0, rb), :], bs)
    left(a_buf.at[pl.ds(0, 3)], as24)
    left(a_buf.at[0, pl.ds(0, 7 * ra), :], as7)
    two.end(PT)
    one.end(ST)


def solution(mesh):
    all_axes = ("depth", "row", "col")

    def device_block(a_rows, b_rows):
        ra, k = a_rows.shape
        rb, n = b_rows.shape
        nb = n // (2 * Y) // BLOCKS
        dma = pltpu.SemaphoreType.DMA
        f32, bf16 = jnp.float32, a_rows.dtype

        def both(*tail, dtype):
            return [pltpu.VMEM((PT, *tail, 2 * nb), dtype), pltpu.VMEM((ST, *tail, nb), dtype)]

        scratch = [
            pltpu.VMEM((Y, 2 * X * ra, k // X), bf16),
            pltpu.VMEM((BLOCKS, 2 * Y, Z * rb, nb), bf16),
            *both(2 * X * ra, dtype=f32),
            *both(ra, dtype=f32), *both(ra, dtype=f32),
            *both(2, ra, dtype=f32), *both(2, ra, dtype=f32),
            *both(2, ra, dtype=bf16),
            dma((2, 4)), dma((2, 4)), dma((2, 4)), dma((2, 4)),
            dma, dma((BLOCKS,)), dma, dma((X,)), dma((2, X)), dma((X,)), dma((Y,)), dma, dma,
            dma, dma((PT,)), dma((PT,)), dma, dma,
            dma, dma((ST,)), dma((ST,)), dma, dma,
        ]
        return pl.pallas_call(
            kernel,
            out_shape=pltpu.VMEM((ra, n), bf16),
            in_specs=[pl.BlockSpec(memory_space=pl.ANY)] * 2,
            out_specs=pl.BlockSpec(memory_space=pltpu.VMEM),
            scratch_shapes=scratch,
            compiler_params=pltpu.CompilerParams(
                collective_id=0, has_side_effects=True, vmem_limit_bytes=62000000),
        )(a_rows, b_rows)

    return jax.shard_map(device_block, mesh=mesh, in_specs=(P(all_axes, None), P(all_axes, None)),
                         out_specs=P(all_axes, None), check_vma=False)
```
